128 devices in a mesh: gx: 16 (over z, y_hi, core), gy: 8 (over y_lo, x).
Axes of the slice: x: 4, y: 4 (y_hi: 2, y_lo: 2; y = y_hi * 2 + y_lo), z: 4, core: 2. Of those that a mesh axis runs over, the one named last changes fastest.
Arguments:
- density: float32 [256, 256, 256], P('gx', 'gy'), may hold values from 0.05 to 2
Outputs:
- potential: float32 [256, 256, 256], P('gx', 'gy')
- energy: float32 [], replicated
The draws below stay inside these ranges and needn't reach their ends.
All inputs are finite; a program needn't handle non-finite values.
Results may differ from the reference program's by a relative error of at most 0.00005.
Values sent between devices are 32-bit elements.
A program may use at most 64 MiB of HBM per device.

```python
import math
import jax
import jax.numpy as jnp

NX = 256
NY = 256
NZ = 256


def block_scale(stream_key, dims, split, least, high):
    gain = 1.0
    for position, blocks in split:
        heights = jax.random.uniform(jax.random.fold_in(jax.random.fold_in(stream_key, 6), position), (blocks,), jnp.float32, least / len(split), high / len(split))
        gain = gain * jnp.repeat(jnp.exp(heights), dims[position] // blocks).reshape((-1,) + (1,) * (len(dims) - 1 - position))
    return gain


def setup_inputs(seed: int = 0) -> dict:
    streams_of = jax.random.split(jax.random.key(seed), 2)
    density = jnp.clip(jnp.exp(math.log(2.0) - 3.6888794 * jax.random.uniform(streams_of[0], (NX, NY, NZ), jnp.float32) ** block_scale(streams_of[0], (NX, NY, NZ), ((0, 16), (1, 8)), -0.2, 0.2)), 0.05, 2.0)
    return dict(density=density)


spacing = 1.0
pbe_kappa = 0.804
pbe_mu = 0.2195149727645171
pbe_beta = 0.06672455060314922
pbe_gamma = 0.031090690869654894
pw_coef = 0.0310907
pw_alpha = 0.2137
pw_first = 7.5957
pw_second = 3.5876
pw_third = 1.6382
pw_fourth = 0.49294

def xc_energy(electrons, grad_sq):
    k_fermi = jnp.cbrt(3.0 * math.pi ** 2 * electrons)
    exch_unif = -0.75 * k_fermi / math.pi
    s_square = grad_sq / (4.0 * k_fermi ** 2 * electrons ** 2)
    enhance = 1.0 + pbe_kappa - pbe_kappa / (1.0 + pbe_mu * s_square / pbe_kappa)
    wigner = jnp.cbrt(3.0 / (4.0 * math.pi * electrons))
    root_rs = jnp.sqrt(wigner)
    series = 2.0 * pw_coef * (pw_first * root_rs + pw_second * wigner + pw_third * wigner * root_rs + pw_fourth * wigner ** 2)
    corr_unif = -2.0 * pw_coef * (1.0 + pw_alpha * wigner) * jnp.log(1.0 + 1.0 / series)
    screen_sq = 4.0 * k_fermi / math.pi
    t_square = grad_sq / (4.0 * screen_sq * electrons ** 2)
    factor = pbe_beta / pbe_gamma / jnp.expm1(-corr_unif / pbe_gamma)
    scaled = factor * t_square
    gradient_term = pbe_gamma * jnp.log(1.0 + pbe_beta / pbe_gamma * t_square * (1.0 + scaled) / (1.0 + scaled + scaled ** 2))
    return electrons * (exch_unif * enhance + corr_unif + gradient_term)

def summed_energy(electrons, grad_sq):
    return jnp.sum(xc_energy(electrons, grad_sq))

def wavenum(count):
    index = jnp.arange(count, dtype=jnp.int32)
    signed = jnp.where(index < count // 2, index, index - count)
    signed = jnp.where(index == count // 2, 0, signed)
    return signed.astype(jnp.float32) * (2.0 * math.pi / (count * spacing))

def reference(density):
    spectrum = jnp.fft.fftn(density)
    waves = (wavenum(NX)[:, None, None], wavenum(NY)[None, :, None], wavenum(NZ)[None, None, :])
    gradients = [jnp.real(jnp.fft.ifftn(1j * wavevec * spectrum)) for wavevec in waves]
    grad_sq = gradients[0] ** 2 + gradients[1] ** 2 + gradients[2] ** 2
    energy_sum, partials = jax.value_and_grad(summed_energy, argnums=(0, 1))(density, grad_sq)
    d_dens, d_grad = partials
    flux_spec = 1j * waves[0] * jnp.fft.fftn(2.0 * d_grad * gradients[0])
    flux_spec = flux_spec + 1j * waves[1] * jnp.fft.fftn(2.0 * d_grad * gradients[1])
    flux_spec = flux_spec + 1j * waves[2] * jnp.fft.fftn(2.0 * d_grad * gradients[2])
    divergence = jnp.real(jnp.fft.ifftn(flux_spec))
    potential = d_dens - divergence
    energy = energy_sum / (NX * NY * NZ)
    return (potential, energy)
```

```python
import functools
import math

import jax
import jax.numpy as jnp
import numpy as np
from jax import lax
from jax.experimental import pallas as pl
from jax.experimental.pallas import tpu as pltpu
from jax.sharding import PartitionSpec as P

MESH = pl.DeviceIdType.MESH
F32 = jnp.float32
BF16 = jnp.bfloat16

N = 256
NJ = 16
NK = 8
ND = NJ * NK
ROWS = N * N * N // ND // 128

pbe_kappa = 0.804
pbe_mu = 0.2195149727645171
pbe_beta = 0.06672455060314922
pbe_gamma = 0.031090690869654894
pw_coef = 0.0310907
pw_alpha = 0.2137
pw_first = 7.5957
pw_second = 3.5876
pw_third = 1.6382
pw_fourth = 0.49294

kf_coef = (3.0 * math.pi**2) ** (1.0 / 3.0)
rs_coef = (3.0 / (4.0 * math.pi)) ** (1.0 / 3.0)


def deriv_matrix():
    m = np.arange(N)
    signed = np.where(m < N // 2, m, m - N)
    signed = np.where(m == N // 2, 0, signed) * (2.0 * math.pi / N)
    shift = (m[:, None] - m[None, :]) % N
    line = -(signed[None, :] * np.sin(2.0 * math.pi * (m[:, None] * m[None, :] % N) / N)).sum(1) / N
    return line[shift]


def row_order():
    r = np.arange(N)
    return 16 * ((r % 64) // 4) + 4 * (r % 4) + r // 64


def split_np(a):
    hi = a.astype(jnp.bfloat16)
    lo = (a - hi.astype(np.float64)).astype(jnp.bfloat16)
    return hi, lo


def split(a):
    hi = a.astype(BF16)
    lo = (a - hi.astype(F32)).astype(BF16)
    return hi, lo


def dot(a, b):
    return jnp.dot(a, b, preferred_element_type=F32)


def matmul(a, b):
    (ah, al), (bh, bl) = a, b
    return dot(ah, bh) + (dot(ah, bl) + dot(al, bh))


def xc_parts(n, g):
    w = jnp.exp2(jnp.log2(n) * (-1.0 / 6.0))
    w2 = w * w
    w4 = w2 * w2
    w8 = w4 * w4
    cube = n * w4
    exch = cube * (-0.75 * kf_coef / math.pi)
    s_n = w8 * w8 * (1.0 / (4.0 * kf_coef**2))
    t_n = w8 * w4 * w2 * (math.pi / (16.0 * kf_coef))
    s_square = g * s_n
    t_square = g * t_n
    quot = 1.0 / (1.0 + (pbe_mu / pbe_kappa) * s_square)
    enhance = (1.0 + pbe_kappa) - pbe_kappa * quot
    exch_slope = exch * (pbe_mu * quot * quot)

    x = w * math.sqrt(rs_coef)
    rs = w2 * rs_coef
    c2 = 2.0 * pw_coef
    series = x * (c2 * pw_first + x * (c2 * pw_second + x * (c2 * pw_third + x * (c2 * pw_fourth))))
    series_rs = x * (
        0.5 * c2 * pw_first + x * (c2 * pw_second + x * (1.5 * c2 * pw_third + x * (2.0 * c2 * pw_fourth)))
    )
    inv_both = 1.0 / (series * (series + 1.0))
    logarithm = jnp.log(1.0 + (series + 1.0) * inv_both)
    lead = c2 + (c2 * pw_alpha) * rs
    corr = -lead * logarithm
    corr_rs = lead * series_rs * inv_both - (c2 * pw_alpha) * rs * logarithm

    grown = jnp.exp(corr * (-1.0 / pbe_gamma))
    inv_e = 1.0 / (grown - 1.0)
    factor = (pbe_beta / pbe_gamma) * inv_e
    y = factor * t_square
    y1 = 1.0 + y
    den = y1 + y * y
    both = den + (pbe_beta / pbe_gamma) * t_square * y1
    inv = 1.0 / (den * both)
    term = pbe_gamma * jnp.log(both * both * inv)
    term_t = pbe_beta * (y1 + y) * inv
    term_c = (-pbe_beta / pbe_gamma) * (t_square * t_square) * (y * (1.0 + y1)) * inv * (factor * grown * inv_e)

    per_cell = exch * enhance + corr + term
    d_dens = (
        per_cell
        + (1.0 / 3.0) * exch * enhance
        - (8.0 / 3.0) * exch_slope * s_square
        - (1.0 / 3.0) * corr_rs * (1.0 + term_c)
        - (7.0 / 3.0) * term_t * t_square
    )
    twice_d_grad = (2.0 * n) * (exch_slope * s_n + term_t * t_n)
    return n * per_cell, d_dens, twice_d_grad


def block_turn(parts):
    group = lax.broadcasted_iota(jnp.int32, parts[0].shape, 1) // 32
    turned = [parts[0]] + [pltpu.roll(parts[b], 32 * b, 1) for b in range(1, 4)]
    out = []
    for a in range(4):
        mixed = jnp.where(
            group < 2,
            jnp.where(group == 0, turned[-a % 4], turned[(1 - a) % 4]),
            jnp.where(group == 2, turned[(2 - a) % 4], turned[(3 - a) % 4]),
        )
        out.append(mixed if a == 0 else pltpu.roll(mixed, 128 - 32 * a, 1))
    return out


def kernel(
    f_hbm, dh_hbm, dl_hbm, xh_hbm, xl_hbm, out_ref, en_ref,
    f_ref, dh_ref, dl_ref, xh_ref, xl_ref,
    send_n, send_g, got_n, got_g, plane_n, plane_x, plane_y, plane_g,
    send_f, send_v, got_f, got_v, e_own, e_row, e_mid, e_all,
    load_sem, send_sem, recv_sem,
):
    j = lax.axis_index("gx")
    k = lax.axis_index("gy")
    me = j * NK + k
    place = k * NJ + j

    loads = [
        pltpu.make_async_copy(src, dst, load_sem.at[i])
        for i, (src, dst) in enumerate(
            ((f_hbm, f_ref), (dh_hbm, dh_ref), (dl_hbm, dl_ref), (xh_hbm, xh_ref), (xl_hbm, xl_ref))
        )
    ]
    for load in loads:
        load.start()

    barrier = pltpu.get_barrier_semaphore()

    def greet(i, carry):
        p = lax.rem(me + i, ND)
        pl.semaphore_signal(barrier, inc=1, device_id=(p // NK, lax.rem(p, NK)), device_id_type=MESH)
        return carry

    lax.fori_loop(1, ND, greet, 0)

    for load in loads:
        load.wait()
    deriv = (dh_ref[...], dl_ref[...])
    deriv_x = (xh_ref[...], xl_ref[...])

    def lay_out(ref, h, block):
        for c in range(2):
            for zz in range(2):
                ref[pl.ds(2 * (2 * h + c) + zz, 128, stride=8), :] = block[
                    128 * zz : 128 * zz + 128, 128 * c : 128 * c + 128
                ]

    for h in range(2):
        turned = f_ref[256 * h : 256 * h + 256, :].T
        lay_out(send_n, h, turned)
        lay_out(send_g, h, matmul(deriv, split(turned)))

    pl.semaphore_wait(barrier, ND - 1)

    def to_planes(src, dst, s):
        def send(i, carry):
            p = lax.rem(me + i, ND)
            pltpu.make_async_remote_copy(
                src_ref=src.at[pl.ds(pl.multiple_of(p * 8, 8), 8)],
                dst_ref=dst.at[pl.ds(pl.multiple_of(place * 8, 8), 8)],
                send_sem=send_sem.at[s],
                recv_sem=recv_sem.at[s],
                device_id=(p // NK, lax.rem(p, NK)),
                device_id_type=MESH,
            ).start()
            return carry

        lax.fori_loop(1, ND, send, 0)
        dst[pl.ds(pl.multiple_of(place * 8, 8), 8), :] = src[pl.ds(pl.multiple_of(me * 8, 8), 8), :]

    def to_home(src, dst, s):
        def send(i, carry):
            p = lax.rem(me + i, ND)
            pj, pk = p // NK, lax.rem(p, NK)
            pltpu.make_async_remote_copy(
                src_ref=src.at[pl.ds(pl.multiple_of((pk * NJ + pj) * 8, 8), 8)],
                dst_ref=dst.at[pl.ds(pl.multiple_of(me * 8, 8), 8)],
                send_sem=send_sem.at[s],
                recv_sem=recv_sem.at[s],
                device_id=(pj, pk),
                device_id_type=MESH,
            ).start()
            return carry

        lax.fori_loop(1, ND, send, 0)
        dst[pl.ds(pl.multiple_of(me * 8, 8), 8), :] = src[pl.ds(pl.multiple_of(place * 8, 8), 8), :]

    def wait_all(ref, sem, rows):
        part = ref.at[pl.ds(0, rows)]
        pltpu.make_async_copy(part, part, sem).wait()

    to_planes(send_n, got_n, 0)
    to_planes(send_g, got_g, 1)

    def unpack(src, dst):
        for zz in range(2):
            for kh in range(2):
                parts = [src[pl.ds((4 * kh + k4) * 128 + zz, 64, stride=2), :] for k4 in range(4)]
                for x4, part in enumerate(block_turn(parts)):
                    dst[zz, 64 * x4 : 64 * x4 + 64, 128 * kh : 128 * kh + 128] = part

    def pack(src, dst):
        for zz in range(2):
            for kh in range(2):
                parts = [src[zz, 64 * x4 : 64 * x4 + 64, 128 * kh : 128 * kh + 128] for x4 in range(4)]
                for k4, part in enumerate(block_turn(parts)):
                    dst[pl.ds((4 * kh + k4) * 128 + zz, 64, stride=2), :] = part

    moved = 8 * (ND - 1)
    wait_all(got_n, recv_sem.at[0], moved)
    unpack(got_n, plane_n)
    for zz in range(2):
        field = split(plane_n[zz])
        plane_x[zz] = matmul(deriv_x, field)
        plane_y[zz] = -matmul(field, deriv)

    wait_all(got_g, recv_sem.at[1], moved)
    unpack(got_g, plane_g)

    step_rows = 16
    total = jnp.zeros((8, 128), F32)
    for zz in range(2):

        def cells(i, total, zz=zz):
            at = pl.ds(pl.multiple_of(i * step_rows, step_rows), step_rows)
            n = plane_n[zz, at, :]
            gx = plane_x[zz, at, :]
            gy = plane_y[zz, at, :]
            gz = plane_g[zz, at, :]
            f, d_dens, slope = xc_parts(n, gx * gx + gy * gy + gz * gz)
            plane_n[zz, at, :] = d_dens
            plane_x[zz, at, :] = slope * gx
            plane_y[zz, at, :] = slope * gy
            plane_g[zz, at, :] = slope * gz
            for a in range(step_rows // 8):
                for b in range(2):
                    total = total + f[8 * a : 8 * a + 8, 128 * b : 128 * b + 128]
            return total

        total = lax.fori_loop(0, N // step_rows, cells, total)

    pack(plane_g, send_f)
    to_home(send_f, got_f, 2)

    mine = jnp.sum(total, axis=0, keepdims=True)
    e_own[0] = mine
    e_row[k] = mine

    def send_row(i, carry):
        pk = lax.rem(k + i, NK)
        pltpu.make_async_remote_copy(
            src_ref=e_own.at[0], dst_ref=e_row.at[k], send_sem=send_sem.at[4], recv_sem=recv_sem.at[4],
            device_id=(j, pk), device_id_type=MESH,
        ).start()
        return carry

    lax.fori_loop(1, NK, send_row, 0)

    for zz in range(2):
        flux_x = split(plane_x[zz])
        flux_y = split(plane_y[zz])
        plane_n[zz] = plane_n[zz] - matmul(deriv_x, flux_x) + matmul(flux_y, deriv)
    pack(plane_n, send_v)
    to_home(send_v, got_v, 3)

    wait_all(e_row, recv_sem.at[4], NK - 1)
    row = jnp.sum(e_row[...], axis=0)
    e_mid[0] = row
    e_all[j] = row

    def send_all(i, carry):
        pj = lax.rem(j + i, NJ)
        pltpu.make_async_remote_copy(
            src_ref=e_mid.at[0], dst_ref=e_all.at[j], send_sem=send_sem.at[5], recv_sem=recv_sem.at[5],
            device_id=(pj, k), device_id_type=MESH,
        ).start()
        return carry

    lax.fori_loop(1, NJ, send_all, 0)

    def gathered(ref, h):
        return jnp.concatenate(
            [
                jnp.concatenate([ref[pl.ds(2 * (2 * h + c) + zz, 128, stride=8), :] for c in range(2)], axis=1)
                for zz in range(2)
            ],
            axis=0,
        )

    wait_all(got_f, recv_sem.at[2], moved)
    for h in range(2):
        plane_x[h] = matmul(deriv, split(gathered(got_f, h)))
    wait_all(got_v, recv_sem.at[3], moved)
    for h in range(2):
        out_ref[256 * h : 256 * h + 256, :] = (gathered(got_v, h) - plane_x[h]).T

    wait_all(e_all, recv_sem.at[5], NJ - 1)
    en_ref[0, 0] = jnp.sum(jnp.sum(e_all[...], axis=0)) * (1.0 / N**3)

    for s, ref in enumerate((send_n, send_g, send_f, send_v)):
        wait_all(ref, send_sem.at[s], moved)
    wait_all(e_row, send_sem.at[4], NK - 1)
    wait_all(e_all, send_sem.at[5], NJ - 1)


def body(density):
    flat = density.reshape(-1, density.shape[2])
    deriv = deriv_matrix()
    order = row_order()
    dh, dl = split_np(deriv)
    xh, xl = split_np(deriv[order][:, order])
    anyspec = pl.BlockSpec(memory_space=pl.ANY)
    lines = pltpu.VMEM((ROWS, 128), F32)
    planes = pltpu.VMEM((2, N, N), F32)
    matrix = pltpu.VMEM((N, N), BF16)
    potential, energy = pl.pallas_call(
        kernel,
        name="pbe",
        out_shape=(
            jax.ShapeDtypeStruct(flat.shape, F32),
            jax.ShapeDtypeStruct((1, 1), F32),
        ),
        in_specs=[anyspec] * 5,
        out_specs=(pl.BlockSpec(memory_space=pltpu.VMEM), pl.BlockSpec(memory_space=pltpu.SMEM)),
        scratch_shapes=[pltpu.VMEM(flat.shape, F32)]
        + [matrix] * 4
        + [lines] * 4
        + [planes] * 4
        + [lines] * 4
        + [
            pltpu.VMEM((1, 1, 128), F32),
            pltpu.VMEM((NK, 1, 128), F32),
            pltpu.VMEM((1, 1, 128), F32),
            pltpu.VMEM((NJ, 1, 128), F32),
            pltpu.SemaphoreType.DMA((5,)),
            pltpu.SemaphoreType.DMA((6,)),
            pltpu.SemaphoreType.DMA((6,)),
        ],
        compiler_params=pltpu.CompilerParams(collective_id=0, has_side_effects=True, vmem_limit_bytes=40 * 2**20),
    )(flat, jnp.asarray(dh), jnp.asarray(dl), jnp.asarray(xh), jnp.asarray(xl))
    return potential.reshape(density.shape), energy[0, 0]


def solution(mesh):
    return jax.shard_map(
        body,
        mesh=mesh,
        in_specs=(P("gx", "gy", None),),
        out_specs=(P("gx", "gy", None), P()),
        check_vma=False,
    )
```

```python
import functools
import math

import jax
import jax.numpy as jnp
import numpy as np
from jax import lax
from jax.experimental import pallas as pl
from jax.experimental.pallas import tpu as pltpu
from jax.sharding import PartitionSpec as P

LOGICAL = pl.DeviceIdType.LOGICAL
UNROLL = 4
F32 = jnp.float32
BF16 = jnp.bfloat16

N = 256
NJ = 16
NK = 8
ND = NJ * NK
ROWS = N * N * N // ND // 128

pbe_kappa = 0.804
pbe_mu = 0.2195149727645171
pbe_beta = 0.06672455060314922
pbe_gamma = 0.031090690869654894
pw_coef = 0.0310907
pw_alpha = 0.2137
pw_first = 7.5957
pw_second = 3.5876
pw_third = 1.6382
pw_fourth = 0.49294

kf_coef = (3.0 * math.pi**2) ** (1.0 / 3.0)
rs_coef = (3.0 / (4.0 * math.pi)) ** (1.0 / 3.0)


def deriv_matrix():
    m = np.arange(N)
    signed = np.where(m < N // 2, m, m - N)
    signed = np.where(m == N // 2, 0, signed) * (2.0 * math.pi / N)
    shift = (m[:, None] - m[None, :]) % N
    line = -(signed[None, :] * np.sin(2.0 * math.pi * (m[:, None] * m[None, :] % N) / N)).sum(1) / N
    return line[shift]


def row_order():
    r = np.arange(N)
    return 16 * ((r % 64) // 4) + 4 * (r % 4) + r // 64


def split_np(a):
    hi = a.astype(jnp.bfloat16)
    lo = (a - hi.astype(np.float64)).astype(jnp.bfloat16)
    return hi, lo


def split(a):
    hi = a.astype(BF16)
    lo = (a - hi.astype(F32)).astype(BF16)
    return hi, lo


def dot(a, b):
    return jnp.dot(a, b, preferred_element_type=F32)


def matmul(a, b):
    (ah, al), (bh, bl) = a, b
    return dot(ah, bh) + (dot(ah, bl) + dot(al, bh))


def xc_parts(n, g):
    w = jnp.exp2(jnp.log2(n) * (-1.0 / 6.0))
    w2 = w * w
    w4 = w2 * w2
    w8 = w4 * w4
    cube = n * w4
    exch = cube * (-0.75 * kf_coef / math.pi)
    s_n = w8 * w8 * (1.0 / (4.0 * kf_coef**2))
    t_n = w8 * w4 * w2 * (math.pi / (16.0 * kf_coef))
    s_square = g * s_n
    t_square = g * t_n
    quot = 1.0 / (1.0 + (pbe_mu / pbe_kappa) * s_square)
    enhance = (1.0 + pbe_kappa) - pbe_kappa * quot
    exch_slope = exch * (pbe_mu * quot * quot)

    x = w * math.sqrt(rs_coef)
    rs = w2 * rs_coef
    c2 = 2.0 * pw_coef
    series = x * (c2 * pw_first + x * (c2 * pw_second + x * (c2 * pw_third + x * (c2 * pw_fourth))))
    series_rs = x * (
        0.5 * c2 * pw_first + x * (c2 * pw_second + x * (1.5 * c2 * pw_third + x * (2.0 * c2 * pw_fourth)))
    )
    inv_both = 1.0 / (series * (series + 1.0))
    logarithm = jnp.log(1.0 + (series + 1.0) * inv_both)
    lead = c2 + (c2 * pw_alpha) * rs
    corr = -lead * logarithm
    corr_rs = lead * series_rs * inv_both - (c2 * pw_alpha) * rs * logarithm

    grown = jnp.exp(corr * (-1.0 / pbe_gamma))
    inv_e = 1.0 / (grown - 1.0)
    factor = (pbe_beta / pbe_gamma) * inv_e
    y = factor * t_square
    y1 = 1.0 + y
    den = y1 + y * y
    both = den + (pbe_beta / pbe_gamma) * t_square * y1
    inv = 1.0 / (den * both)
    term = pbe_gamma * jnp.log(both * both * inv)
    term_t = pbe_beta * (y1 + y) * inv
    term_c = (-pbe_beta / pbe_gamma) * (t_square * t_square) * (y * (1.0 + y1)) * inv * (factor * grown * inv_e)

    per_cell = exch * enhance + corr + term
    d_dens = (
        per_cell
        + (1.0 / 3.0) * exch * enhance
        - (8.0 / 3.0) * exch_slope * s_square
        - (1.0 / 3.0) * corr_rs * (1.0 + term_c)
        - (7.0 / 3.0) * term_t * t_square
    )
    twice_d_grad = (2.0 * n) * (exch_slope * s_n + term_t * t_n)
    return n * per_cell, d_dens, twice_d_grad


def block_turn(parts):
    group = lax.broadcasted_iota(jnp.int32, parts[0].shape, 1) // 32
    turned = [parts[0]] + [pltpu.roll(parts[b], 32 * b, 1) for b in range(1, 4)]
    out = []
    for a in range(4):
        mixed = jnp.where(
            group < 2,
            jnp.where(group == 0, turned[-a % 4], turned[(1 - a) % 4]),
            jnp.where(group == 2, turned[(2 - a) % 4], turned[(3 - a) % 4]),
        )
        out.append(mixed if a == 0 else pltpu.roll(mixed, 128 - 32 * a, 1))
    return out


def kernel(
    f_hbm, mats_hbm, out_ref, en_ref,
    f_ref, mats,
    send_n, send_g, got_n, got_g, plane_n, plane_x, plane_y,
    send_f, send_v, got_f, got_v, e_own, e_row, e_mid, e_all,
    load_sem, send_sem, recv_sem, chunk_sem,
):
    j = lax.axis_index("gx")
    k = lax.axis_index("gy")
    me = j * NK + k
    mine_jp = j // 2
    low = me % 16
    chunks = NJ // 2

    def place_of(p):
        return pl.multiple_of(((p & 112) + ((p & 7) << 1) + ((p >> 3) & 1)) * 8, 8)

    load_f = pltpu.make_async_copy(f_hbm, f_ref, load_sem.at[0])
    load_m = pltpu.make_async_copy(mats_hbm, mats, load_sem.at[1])
    load_f.start()
    load_m.start()

    barrier = pltpu.get_barrier_semaphore()

    def greet(i, carry):
        pl.semaphore_signal(barrier, inc=1, device_id=(me + i) & (ND - 1), device_id_type=LOGICAL)
        return carry

    with jax.named_scope("greet"):
        lax.fori_loop(1, ND, greet, 0, unroll=UNROLL)

    def lay_out(ref, h, block):
        for c in range(2):
            for zz in range(2):
                ref[pl.ds(2 * (2 * h + c) + zz, 128, stride=8), :] = block[
                    128 * zz : 128 * zz + 128, 128 * c : 128 * c + 128
                ]

    def send_to(p, src, dst, s, r):
        pltpu.make_async_remote_copy(
            src_ref=src, dst_ref=dst, send_sem=send_sem.at[s], recv_sem=r, device_id=p, device_id_type=LOGICAL
        ).start()

    def to_planes(src, dst, s, r):
        here = dst.at[pl.ds(place_of(me), 8)]

        def send(t, carry):
            p = (((mine_jp + 1) * 16 + t) & 112) + ((low + t) & 15)
            send_to(p, src.at[pl.ds(pl.multiple_of(p * 8, 8), 8)], here, s, r)
            return carry

        lax.fori_loop(0, ND - 16, send, 0, unroll=UNROLL)
        lax.fori_loop(ND - 15, ND, send, 0, unroll=UNROLL)
        dst[pl.ds(place_of(me), 8), :] = src[pl.ds(pl.multiple_of(me * 8, 8), 8), :]

    def to_home_one(p, src, dst, s):
        send_to(
            p,
            src.at[pl.ds(place_of(p), 8)],
            dst.at[pl.ds(pl.multiple_of(me * 8, 8), 8)],
            s,
            recv_sem.at[s],
        )

    def wait_all(ref, sem, rows):
        part = ref.at[pl.ds(0, rows)]
        pltpu.make_async_copy(part, part, sem).wait()

    with jax.named_scope("load"):
        load_f.wait()
        turned = [f_ref[256 * h : 256 * h + 256, :].T for h in range(2)]
        for h in range(2):
            lay_out(send_n, h, turned[h])
    with jax.named_scope("barrier"):
        pl.semaphore_wait(barrier, ND - 1)
    with jax.named_scope("send_n"):
        to_planes(send_n, got_n, 0, recv_sem.at[0])
    with jax.named_scope("grad_z"):
        load_m.wait()
        deriv = (mats[0], mats[1])
        deriv_x = (mats[2], mats[3])
        for h in range(2):
            lay_out(send_g, h, matmul(deriv, split(turned[h])))
    with jax.named_scope("send_g"):
        to_planes(send_g, got_g, 1, chunk_sem.at[mine_jp])

    moved = 8 * (ND - 1)
    with jax.named_scope("wait_n"):
        wait_all(got_n, recv_sem.at[0], moved)

    def pieces(src, jp, zz, kh):
        base = jp * 128 + kh * 64 + zz
        return block_turn([src[pl.ds(base + 16 * k4, 8, stride=2), :] for k4 in range(4)])

    with jax.named_scope("grad_xy"):
        for zz in range(2):
            for kh in range(2):
                for jp in range(chunks):
                    for x4, part in enumerate(pieces(got_n, jp, zz, kh)):
                        plane_n[zz, 64 * x4 + 8 * jp : 64 * x4 + 8 * jp + 8, 128 * kh : 128 * kh + 128] = part
        for zz in range(2):
            field = split(plane_n[zz])
            plane_x[zz] = matmul(deriv_x, field)
            plane_y[zz] = -matmul(field, deriv)

    def cells(i, total):
        jp = (mine_jp + chunks - 1 - i) & (chunks - 1)

        @pl.when(i < chunks - 1)
        def _():
            wait_all(got_g, chunk_sem.at[jp], 128)

        @pl.when(i == chunks - 1)
        def _():
            wait_all(got_g, chunk_sem.at[jp], 120)

        at = [pl.ds(pl.multiple_of(64 * x4 + 8 * jp, 8), 8) for x4 in range(4)]
        base = pl.multiple_of(jp * 128, 128)
        for group in [[(zz, kh) for kh in range(2)] for zz in range(2)]:
            refs = [
                (zz, at[x4], slice(128 * kh, 128 * kh + 128)) for zz, kh in group for x4 in range(4)
            ]
            n = jnp.concatenate([plane_n[r] for r in refs], axis=0)
            gx = jnp.concatenate([plane_x[r] for r in refs], axis=0)
            gy = jnp.concatenate([plane_y[r] for r in refs], axis=0)
            gz = jnp.concatenate(
                [
                    part
                    for zz, kh in group
                    for part in block_turn(
                        [got_g[pl.ds(base + (kh * 64 + zz + 16 * k4), 8, stride=2), :] for k4 in range(4)]
                    )
                ],
                axis=0,
            )
            f, d_dens, slope = xc_parts(n, gx * gx + gy * gy + gz * gz)
            fx, fy, fz = slope * gx, slope * gy, slope * gz
            for g, (zz, kh) in enumerate(group):
                parts = block_turn([fz[32 * g + 8 * x4 : 32 * g + 8 * x4 + 8] for x4 in range(4)])
                for k4, part in enumerate(parts):
                    send_f[pl.ds(base + (kh * 64 + zz + 16 * k4), 8, stride=2), :] = part
            for i8, r in enumerate(refs):
                plane_n[r] = d_dens[8 * i8 : 8 * i8 + 8]
                plane_x[r] = fx[8 * i8 : 8 * i8 + 8]
                plane_y[r] = fy[8 * i8 : 8 * i8 + 8]
                total = total + f[8 * i8 : 8 * i8 + 8]

        def send(q, carry):
            p = jp * 16 + ((low + 16 - q) & 15)
            to_home_one(p, send_f, got_f, 2)
            return carry

        @pl.when(i < chunks - 1)
        def _():
            send(0, 0)

        lax.fori_loop(1, 16, send, 0, unroll=UNROLL)
        return total

    with jax.named_scope("cells"):
        total = lax.fori_loop(0, chunks, cells, jnp.zeros((8, 128), F32))
        mine = jnp.sum(total, axis=0, keepdims=True)
        e_own[0] = mine
        e_row[k] = mine
        got_f[pl.ds(pl.multiple_of(me * 8, 8), 8), :] = send_f[pl.ds(place_of(me), 8), :]

    def send_row(i, carry):
        send_to(j * NK + ((k + i) & (NK - 1)), e_own.at[0], e_row.at[k], 4, recv_sem.at[4])
        return carry

    lax.fori_loop(1, NK, send_row, 0)

    with jax.named_scope("divergence"):
        for zz in range(2):
            flux_x = split(plane_x[zz])
            flux_y = split(plane_y[zz])
            plane_n[zz] = plane_n[zz] - matmul(deriv_x, flux_x) + matmul(flux_y, deriv)
        for zz in range(2):
            for kh in range(2):
                for jp in range(chunks):
                    parts = block_turn(
                        [plane_n[zz, 64 * x4 + 8 * jp : 64 * x4 + 8 * jp + 8, 128 * kh : 128 * kh + 128] for x4 in range(4)]
                    )
                    for k4, part in enumerate(parts):
                        send_v[pl.ds(jp * 128 + kh * 64 + zz + 16 * k4, 8, stride=2), :] = part

    def send_rest(t, carry):
        p = (((mine_jp + chunks - 1) * 16 - (t & 112)) & 112) + ((low + ND - t) & 15)
        to_home_one(p, send_v, got_v, 3)
        return carry

    with jax.named_scope("send_v"):
        lax.fori_loop(0, ND - 16, send_rest, 0, unroll=UNROLL)
        lax.fori_loop(ND - 15, ND, send_rest, 0, unroll=UNROLL)
        got_v[pl.ds(pl.multiple_of(me * 8, 8), 8), :] = send_v[pl.ds(place_of(me), 8), :]

    with jax.named_scope("energy_row"):
        wait_all(e_row, recv_sem.at[4], NK - 1)
        row = jnp.sum(e_row[...], axis=0)
        e_mid[0] = row
        e_all[j] = row

        def send_all(i, carry):
            send_to(((j + i) & (NJ - 1)) * NK + k, e_mid.at[0], e_all.at[j], 5, recv_sem.at[5])
            return carry

        lax.fori_loop(1, NJ, send_all, 0)

    def gathered(ref, h):
        return jnp.concatenate(
            [
                jnp.concatenate([ref[pl.ds(2 * (2 * h + c) + zz, 128, stride=8), :] for c in range(2)], axis=1)
                for zz in range(2)
            ],
            axis=0,
        )

    with jax.named_scope("wait_f"):
        wait_all(got_f, recv_sem.at[2], moved)
    with jax.named_scope("div_z"):
        for h in range(2):
            plane_x[h] = matmul(deriv, split(gathered(got_f, h)))
        wait_all(e_all, recv_sem.at[5], NJ - 1)
        en_ref[0, 0] = jnp.sum(jnp.sum(e_all[...], axis=0)) * (1.0 / N**3)
    with jax.named_scope("wait_v"):
        wait_all(got_v, recv_sem.at[3], moved)
    with jax.named_scope("finish"):
        for h in range(2):
            out_ref[256 * h : 256 * h + 256, :] = (gathered(got_v, h) - plane_x[h]).T

        for s, ref in enumerate((send_n, send_g, send_f, send_v)):
            wait_all(ref, send_sem.at[s], moved)
        wait_all(e_row, send_sem.at[4], NK - 1)
        wait_all(e_all, send_sem.at[5], NJ - 1)


def body(density):
    flat = density.reshape(-1, density.shape[2])
    deriv = deriv_matrix()
    order = row_order()
    mats = np.stack(split_np(deriv) + split_np(deriv[order][:, order]))
    hbm = pl.BlockSpec(memory_space=pltpu.HBM)
    lines = pltpu.VMEM((ROWS, 128), F32)
    planes = pltpu.VMEM((2, N, N), F32)
    potential, energy = pl.pallas_call(
        kernel,
        name="pbe",
        out_shape=(
            jax.ShapeDtypeStruct(flat.shape, F32),
            jax.ShapeDtypeStruct((1, 1), F32),
        ),
        in_specs=[hbm] * 2,
        out_specs=(pl.BlockSpec(memory_space=pltpu.VMEM), pl.BlockSpec(memory_space=pltpu.SMEM)),
        scratch_shapes=[pltpu.VMEM(flat.shape, F32), pltpu.VMEM((4, N, N), BF16)]
        + [lines] * 4
        + [planes] * 3
        + [lines] * 4
        + [
            pltpu.VMEM((1, 1, 128), F32),
            pltpu.VMEM((NK, 1, 128), F32),
            pltpu.VMEM((1, 1, 128), F32),
            pltpu.VMEM((NJ, 1, 128), F32),
            pltpu.SemaphoreType.DMA((2,)),
            pltpu.SemaphoreType.DMA((6,)),
            pltpu.SemaphoreType.DMA((6,)),
            pltpu.SemaphoreType.DMA((NJ // 2,)),
        ],
        compiler_params=pltpu.CompilerParams(collective_id=0, has_side_effects=True, vmem_limit_bytes=40 * 2**20),
    )(*(pltpu.with_memory_space_constraint(a, pltpu.HBM) for a in (flat, jnp.asarray(mats))))
    return potential.reshape(density.shape), energy[0, 0]


def solution(mesh):
    return jax.shard_map(
        body,
        mesh=mesh,
        in_specs=(P("gx", "gy", None),),
        out_specs=(P("gx", "gy", None), P()),
        check_vma=False,
    )
```

```python
import functools
import math

import jax
import jax.numpy as jnp
import numpy as np
from jax import lax
from jax.experimental import pallas as pl
from jax.experimental.pallas import tpu as pltpu
from jax.sharding import PartitionSpec as P

LOGICAL = pl.DeviceIdType.LOGICAL
F32 = jnp.float32
BF16 = jnp.bfloat16

N = 256
NJ = 16
NK = 8
ND = NJ * NK
ROWS = N * N * N // ND // 128

pbe_kappa = 0.804
pbe_mu = 0.2195149727645171
pbe_beta = 0.06672455060314922
pbe_gamma = 0.031090690869654894
pw_coef = 0.0310907
pw_alpha = 0.2137
pw_first = 7.5957
pw_second = 3.5876
pw_third = 1.6382
pw_fourth = 0.49294

kf_coef = (3.0 * math.pi**2) ** (1.0 / 3.0)
rs_coef = (3.0 / (4.0 * math.pi)) ** (1.0 / 3.0)


def deriv_matrix():
    m = np.arange(N)
    signed = np.where(m < N // 2, m, m - N)
    signed = np.where(m == N // 2, 0, signed) * (2.0 * math.pi / N)
    shift = (m[:, None] - m[None, :]) % N
    line = -(signed[None, :] * np.sin(2.0 * math.pi * (m[:, None] * m[None, :] % N) / N)).sum(1) / N
    return line[shift]


def row_order():
    r = np.arange(N)
    return 16 * ((r % 64) // 4) + 4 * (r % 4) + r // 64


def split_np(a):
    hi = a.astype(jnp.bfloat16)
    lo = (a - hi.astype(np.float64)).astype(jnp.bfloat16)
    return hi, lo


def split(a):
    hi = a.astype(BF16)
    lo = (a - hi.astype(F32)).astype(BF16)
    return hi, lo


def dot(a, b):
    return jnp.dot(a, b, preferred_element_type=F32)


def matmul(a, b):
    (ah, al), (bh, bl) = a, b
    return dot(ah, bh) + (dot(ah, bl) + dot(al, bh))


def xc_parts(n, g):
    w = jnp.exp2(jnp.log2(n) * (-1.0 / 6.0))
    w2 = w * w
    w4 = w2 * w2
    w8 = w4 * w4
    cube = n * w4
    exch = cube * (-0.75 * kf_coef / math.pi)
    s_n = w8 * w8 * (1.0 / (4.0 * kf_coef**2))
    t_n = w8 * w4 * w2 * (math.pi / (16.0 * kf_coef))
    s_square = g * s_n
    t_square = g * t_n
    quot = 1.0 / (1.0 + (pbe_mu / pbe_kappa) * s_square)
    enhance = (1.0 + pbe_kappa) - pbe_kappa * quot
    exch_slope = exch * (pbe_mu * quot * quot)

    x = w * math.sqrt(rs_coef)
    rs = w2 * rs_coef
    c2 = 2.0 * pw_coef
    series = x * (c2 * pw_first + x * (c2 * pw_second + x * (c2 * pw_third + x * (c2 * pw_fourth))))
    series_rs = x * (
        0.5 * c2 * pw_first + x * (c2 * pw_second + x * (1.5 * c2 * pw_third + x * (2.0 * c2 * pw_fourth)))
    )
    inv_both = 1.0 / (series * (series + 1.0))
    logarithm = jnp.log(1.0 + (series + 1.0) * inv_both)
    lead = c2 + (c2 * pw_alpha) * rs
    corr = -lead * logarithm
    corr_rs = lead * series_rs * inv_both - (c2 * pw_alpha) * rs * logarithm

    grown = jnp.exp(corr * (-1.0 / pbe_gamma))
    inv_e = 1.0 / (grown - 1.0)
    factor = (pbe_beta / pbe_gamma) * inv_e
    y = factor * t_square
    y1 = 1.0 + y
    den = y1 + y * y
    both = den + (pbe_beta / pbe_gamma) * t_square * y1
    inv = 1.0 / (den * both)
    term = pbe_gamma * jnp.log(both * both * inv)
    term_t = pbe_beta * (y1 + y) * inv
    term_c = (-pbe_beta / pbe_gamma) * (t_square * t_square) * (y * (1.0 + y1)) * inv * (factor * grown * inv_e)

    per_cell = exch * enhance + corr + term
    d_dens = (
        per_cell
        + (1.0 / 3.0) * exch * enhance
        - (8.0 / 3.0) * exch_slope * s_square
        - (1.0 / 3.0) * corr_rs * (1.0 + term_c)
        - (7.0 / 3.0) * term_t * t_square
    )
    twice_d_grad = (2.0 * n) * (exch_slope * s_n + term_t * t_n)
    return n * per_cell, d_dens, twice_d_grad


def block_turn(parts):
    group = lax.broadcasted_iota(jnp.int32, parts[0].shape, 1) // 32
    turned = [parts[0]] + [pltpu.roll(parts[b], 32 * b, 1) for b in range(1, 4)]
    out = []
    for a in range(4):
        mixed = jnp.where(
            group < 2,
            jnp.where(group == 0, turned[-a % 4], turned[(1 - a) % 4]),
            jnp.where(group == 2, turned[(2 - a) % 4], turned[(3 - a) % 4]),
        )
        out.append(mixed if a == 0 else pltpu.roll(mixed, 128 - 32 * a, 1))
    return out


FAR_FIRST = (2, 1, 3, 0)
CHUNKS = 8


def kernel(
    f_hbm, mats_hbm, out_ref, en_ref,
    f_ref, mats,
    send_n, send_g, got_n, got_g, plane_n, plane_x, plane_y, plane_d,
    send_f, send_v, got_f, got_v, div_z, e_own, e_row, e_mid, e_all,
    load_sem, send_sem, recv_sem, chunk_sem,
):
    j = lax.axis_index("gx")
    k = lax.axis_index("gy")
    me = j * NK + k
    own = pl.ds(pl.multiple_of(me * 8, 8), 8)
    chip_z, core, chip_x = j >> 2, j & 1, k & 3
    chip_y = (j & 2) + (k >> 2)
    at_z = [((chip_z + d) & 3) << 5 for d in range(4)]
    at_x = [(chip_x + d) & 3 for d in range(4)]

    def at_y(d):
        y = (chip_y + d) & 3
        return ((y & 2) << 3) + ((y & 1) << 2)

    load_f = pltpu.make_async_copy(f_hbm, f_ref, load_sem.at[0])
    load_m = pltpu.make_async_copy(mats_hbm, mats, load_sem.at[1])
    load_f.start()
    load_m.start()

    barrier = pltpu.get_barrier_semaphore()
    with jax.named_scope("greet"):
        all_y = [at_y(d) for d in range(4)]
        cores = [core << 3, (1 - core) << 3]
        steps = [(dz, dy, dx, dc) for dz in range(4) for dy in range(4) for dx in range(4) for dc in range(2)][1:]
        steps = sorted(steps, key=lambda s: (-sum(min(d, 4 - d) for d in s[:3]), s))
        for dz, dy, dx, dc in steps:
            p = at_z[dz] + all_y[dy] + cores[dc] + at_x[dx]
            pl.semaphore_signal(barrier, inc=1, device_id=p, device_id_type=LOGICAL)

    def chunk_at(i, sign):
        turn = i + 1
        side = (core ^ ((turn >> 2) & 1)) << 3
        return [(d, at_z[sign * d % 4] + at_y(sign * (d + turn)) + side) for d in FAR_FIRST]

    def send_chunk(i, sign, last, one):
        for d, base in chunk_at(i, sign):
            for dx in FAR_FIRST:
                if not (last and d == 0 and dx == 0):
                    one(base + at_x[dx])

    def send_to(p, src, dst, s, r):
        pltpu.make_async_remote_copy(
            src_ref=src, dst_ref=dst, send_sem=send_sem.at[s], recv_sem=r, device_id=p, device_id_type=LOGICAL
        ).start()

    def piece(ref, p):
        return ref.at[pl.ds(pl.multiple_of(p * 8, 8), 8)]

    def send_all_chunks(src, dst, s, sem_of, sign):
        def chunk(i, carry):
            send_chunk(i, sign, False, lambda p: send_to(p, piece(src, p), dst.at[own], s, sem_of(i)))
            return carry

        lax.fori_loop(0, CHUNKS - 1, chunk, 0)
        i = CHUNKS - 1
        send_chunk(i, sign, True, lambda p: send_to(p, piece(src, p), dst.at[own], s, sem_of(i)))
        dst[own, :] = src[own, :]

    def wait_all(ref, sem, rows):
        part = ref.at[pl.ds(0, rows)]
        pltpu.make_async_copy(part, part, sem).wait()

    def lay_out(ref, h, block):
        for c in range(2):
            for zz in range(2):
                ref[pl.ds(2 * (2 * h + c) + zz, 128, stride=8), :] = block[
                    128 * zz : 128 * zz + 128, 128 * c : 128 * c + 128
                ]

    with jax.named_scope("load"):
        load_f.wait()
        turned = [f_ref[256 * h : 256 * h + 256, :].T for h in range(2)]
        for h in range(2):
            lay_out(send_n, h, turned[h])
    with jax.named_scope("barrier"):
        pl.semaphore_wait(barrier, ND - 1)
    with jax.named_scope("send_n"):
        send_all_chunks(send_n, got_n, 0, lambda i: recv_sem.at[0], 1)
    with jax.named_scope("grad_z"):
        load_m.wait()
        deriv = (mats[0], mats[1])
        deriv_x = (mats[2], mats[3])
        for h in range(2):
            lay_out(send_g, h, matmul(deriv, split(turned[h])))
    with jax.named_scope("send_g"):
        send_all_chunks(send_g, got_g, 1, lambda i: chunk_sem.at[i], 1)

    moved = 8 * (ND - 1)
    with jax.named_scope("wait_n"):
        wait_all(got_n, recv_sem.at[0], moved)

    def quad(ref, jk):
        return block_turn([ref[pl.ds(pl.multiple_of(jk * 32 + 8 * k4, 8), 8), :] for k4 in range(4)])

    def plane_of(ref, zz):
        return jnp.concatenate([ref[kh, pl.ds(zz, N, stride=2), :] for kh in range(2)], axis=1)

    with jax.named_scope("grad_xy"):
        for jk in range(2 * NJ):
            for x4, part in enumerate(quad(got_n, jk)):
                plane_n[jk % 2, 128 * x4 + 8 * (jk // 2) : 128 * x4 + 8 * (jk // 2) + 8, :] = part
        for zz in range(2):
            field = split(plane_of(plane_n, zz))
            along_x = matmul(deriv_x, field)
            along_y = matmul(field, deriv)
            for kh in range(2):
                plane_x[kh, pl.ds(zz, N, stride=2), :] = along_x[:, 128 * kh : 128 * kh + 128]
                plane_y[kh, pl.ds(zz, N, stride=2), :] = -along_y[:, 128 * kh : 128 * kh + 128]

    def cells(i, total, last):
        wait_all(got_g, chunk_sem.at[i], 120 if last else 128)
        quads = [base >> 2 for _, base in chunk_at(i, -1)]
        for group in (quads[:2], quads[2:]):
            refs = [
                (jk & 1, pl.ds(pl.multiple_of(128 * x4 + (jk >> 1) * 8, 8), 8), slice(None))
                for jk in group
                for x4 in range(4)
            ]
            n = jnp.concatenate([plane_n[r] for r in refs], axis=0)
            gx = jnp.concatenate([plane_x[r] for r in refs], axis=0)
            gy = jnp.concatenate([plane_y[r] for r in refs], axis=0)
            gz = jnp.concatenate([part for jk in group for part in quad(got_g, jk)], axis=0)
            f, d_dens, slope = xc_parts(n, gx * gx + gy * gy + gz * gz)
            fx, fy, fz = slope * gx, slope * gy, slope * gz
            for g, jk in enumerate(group):
                parts = block_turn([fz[32 * g + 8 * x4 : 32 * g + 8 * x4 + 8] for x4 in range(4)])
                for k4, part in enumerate(parts):
                    send_f[pl.ds(pl.multiple_of(jk * 32 + 8 * k4, 8), 8), :] = part
            for i8, r in enumerate(refs):
                plane_d[r] = d_dens[8 * i8 : 8 * i8 + 8]
                plane_x[r] = fx[8 * i8 : 8 * i8 + 8]
                plane_y[r] = fy[8 * i8 : 8 * i8 + 8]
                total = total + f[8 * i8 : 8 * i8 + 8]
        send_chunk(i, -1, last, lambda p: send_to(p, piece(send_f, p), got_f.at[own], 2, recv_sem.at[2]))
        return total

    with jax.named_scope("cells"):
        total = lax.fori_loop(0, CHUNKS - 1, functools.partial(cells, last=False), jnp.zeros((8, 128), F32))
        total = cells(CHUNKS - 1, total, last=True)
        mine = jnp.sum(total, axis=0, keepdims=True)
        e_own[0] = mine
        e_row[k] = mine
        got_f[own, :] = send_f[own, :]

    def send_row(i, carry):
        send_to(j * NK + ((k + i) & (NK - 1)), e_own.at[0], e_row.at[k], 4, recv_sem.at[4])
        return carry

    lax.fori_loop(1, NK, send_row, 0)

    with jax.named_scope("divergence"):
        for zz in range(2):
            along = matmul(deriv_x, split(plane_of(plane_x, zz))) - matmul(split(plane_of(plane_y, zz)), deriv)
            for kh in range(2):
                rows = (kh, pl.ds(zz, N, stride=2), slice(None))
                plane_d[rows] = plane_d[rows] - along[:, 128 * kh : 128 * kh + 128]
        for jk in range(2 * NJ):
            parts = block_turn(
                [plane_d[jk % 2, 128 * x4 + 8 * (jk // 2) : 128 * x4 + 8 * (jk // 2) + 8, :] for x4 in range(4)]
            )
            for k4, part in enumerate(parts):
                send_v[jk * 32 + 8 * k4 : jk * 32 + 8 * k4 + 8, :] = part

    with jax.named_scope("send_v"):
        send_all_chunks(send_v, got_v, 3, lambda i: recv_sem.at[3], -1)

    with jax.named_scope("energy_row"):
        wait_all(e_row, recv_sem.at[4], NK - 1)
        row = jnp.sum(e_row[...], axis=0)
        e_mid[0] = row
        e_all[j] = row

        def send_col(i, carry):
            send_to(((j + i) & (NJ - 1)) * NK + k, e_mid.at[0], e_all.at[j], 5, recv_sem.at[5])
            return carry

        lax.fori_loop(1, NJ, send_col, 0)

    def gathered(ref, h):
        return jnp.concatenate(
            [
                jnp.concatenate([ref[pl.ds(2 * (2 * h + c) + zz, 128, stride=8), :] for c in range(2)], axis=1)
                for zz in range(2)
            ],
            axis=0,
        )

    with jax.named_scope("wait_f"):
        wait_all(got_f, recv_sem.at[2], moved)
    with jax.named_scope("div_z"):
        for h in range(2):
            div_z[h] = matmul(deriv, split(gathered(got_f, h)))
    with jax.named_scope("wait_v"):
        wait_all(got_v, recv_sem.at[3], moved)
    with jax.named_scope("finish"):
        for h in range(2):
            out_ref[256 * h : 256 * h + 256, :] = (gathered(got_v, h) - div_z[h]).T

    with jax.named_scope("energy"):
        wait_all(e_all, recv_sem.at[5], NJ - 1)
        en_ref[0, 0] = jnp.sum(jnp.sum(e_all[...], axis=0)) * (1.0 / N**3)
        for s, ref in enumerate((send_n, send_g, send_f, send_v)):
            wait_all(ref, send_sem.at[s], moved)
        wait_all(e_row, send_sem.at[4], NK - 1)
        wait_all(e_all, send_sem.at[5], NJ - 1)


def body(density):
    flat = density.reshape(-1, density.shape[2])
    deriv = deriv_matrix()
    order = row_order()
    mats = np.stack(split_np(deriv) + split_np(deriv[order][:, order]))
    hbm = pl.BlockSpec(memory_space=pltpu.HBM)
    lines = pltpu.VMEM((ROWS, 128), F32)
    planes = pltpu.VMEM((2, 2 * N, 128), F32)
    potential, energy = pl.pallas_call(
        kernel,
        name="pbe",
        out_shape=(
            jax.ShapeDtypeStruct(flat.shape, F32),
            jax.ShapeDtypeStruct((1, 1), F32),
        ),
        in_specs=[hbm] * 2,
        out_specs=(pl.BlockSpec(memory_space=pltpu.VMEM), pl.BlockSpec(memory_space=pltpu.SMEM)),
        scratch_shapes=[pltpu.VMEM(flat.shape, F32), pltpu.VMEM((4, N, N), BF16)]
        + [lines] * 4
        + [planes] * 4
        + [lines] * 4
        + [
            pltpu.VMEM((2, N, N), F32),
            pltpu.VMEM((1, 1, 128), F32),
            pltpu.VMEM((NK, 1, 128), F32),
            pltpu.VMEM((1, 1, 128), F32),
            pltpu.VMEM((NJ, 1, 128), F32),
            pltpu.SemaphoreType.DMA((2,)),
            pltpu.SemaphoreType.DMA((6,)),
            pltpu.SemaphoreType.DMA((6,)),
            pltpu.SemaphoreType.DMA((NJ // 2,)),
        ],
        compiler_params=pltpu.CompilerParams(collective_id=0, has_side_effects=True, vmem_limit_bytes=40 * 2**20),
    )(*(pltpu.with_memory_space_constraint(a, pltpu.HBM) for a in (flat, jnp.asarray(mats))))
    return potential.reshape(density.shape), energy[0, 0]


def solution(mesh):
    return jax.shard_map(
        body,
        mesh=mesh,
        in_specs=(P("gx", "gy", None),),
        out_specs=(P("gx", "gy", None), P()),
        check_vma=False,
    )
```

```python
import functools
import math

import jax
import jax.numpy as jnp
import numpy as np
from jax import lax
from jax.experimental import pallas as pl
from jax.experimental.pallas import tpu as pltpu
from jax.sharding import PartitionSpec as P

LOGICAL = pl.DeviceIdType.LOGICAL
F32 = jnp.float32
BF16 = jnp.bfloat16

N = 256
NJ = 16
NK = 8
ND = NJ * NK
ROWS = N * N * N // ND // 128

pbe_kappa = 0.804
pbe_mu = 0.2195149727645171
pbe_beta = 0.06672455060314922
pbe_gamma = 0.031090690869654894
pw_coef = 0.0310907
pw_alpha = 0.2137
pw_first = 7.5957
pw_second = 3.5876
pw_third = 1.6382
pw_fourth = 0.49294

kf_coef = (3.0 * math.pi**2) ** (1.0 / 3.0)
rs_coef = (3.0 / (4.0 * math.pi)) ** (1.0 / 3.0)


def deriv_matrix():
    m = np.arange(N)
    signed = np.where(m < N // 2, m, m - N)
    signed = np.where(m == N // 2, 0, signed) * (2.0 * math.pi / N)
    shift = (m[:, None] - m[None, :]) % N
    line = -(signed[None, :] * np.sin(2.0 * math.pi * (m[:, None] * m[None, :] % N) / N)).sum(1) / N
    return line[shift]


def row_order():
    r = np.arange(N)
    return 16 * ((r % 64) // 4) + 4 * (r % 4) + r // 64


def split_np(a):
    hi = a.astype(jnp.bfloat16)
    lo = (a - hi.astype(np.float64)).astype(jnp.bfloat16)
    return hi, lo


def split(a):
    hi = a.astype(BF16)
    lo = (a - hi.astype(F32)).astype(BF16)
    return hi, lo


def dot(a, b):
    return jnp.dot(a, b, preferred_element_type=F32)


def matmul(a, b):
    (ah, al), (bh, bl) = a, b
    return dot(ah, bh) + (dot(ah, bl) + dot(al, bh))


def xc_parts(n, g):
    w = jnp.exp2(jnp.log2(n) * (-1.0 / 6.0))
    w2 = w * w
    w4 = w2 * w2
    w8 = w4 * w4
    cube = n * w4
    exch = cube * (-0.75 * kf_coef / math.pi)
    s_n = w8 * w8 * (1.0 / (4.0 * kf_coef**2))
    t_n = w8 * w4 * w2 * (math.pi / (16.0 * kf_coef))
    s_square = g * s_n
    t_square = g * t_n
    quot = 1.0 / (1.0 + (pbe_mu / pbe_kappa) * s_square)
    enhance = (1.0 + pbe_kappa) - pbe_kappa * quot
    exch_slope = exch * (pbe_mu * quot * quot)

    x = w * math.sqrt(rs_coef)
    rs = w2 * rs_coef
    c2 = 2.0 * pw_coef
    series = x * (c2 * pw_first + x * (c2 * pw_second + x * (c2 * pw_third + x * (c2 * pw_fourth))))
    series_rs = x * (
        0.5 * c2 * pw_first + x * (c2 * pw_second + x * (1.5 * c2 * pw_third + x * (2.0 * c2 * pw_fourth)))
    )
    inv_both = 1.0 / (series * (series + 1.0))
    logarithm = jnp.log(1.0 + (series + 1.0) * inv_both)
    lead = c2 + (c2 * pw_alpha) * rs
    corr = -lead * logarithm
    corr_rs = lead * series_rs * inv_both - (c2 * pw_alpha) * rs * logarithm

    grown = jnp.exp(corr * (-1.0 / pbe_gamma))
    inv_e = 1.0 / (grown - 1.0)
    factor = (pbe_beta / pbe_gamma) * inv_e
    y = factor * t_square
    y1 = 1.0 + y
    den = y1 + y * y
    both = den + (pbe_beta / pbe_gamma) * t_square * y1
    inv = 1.0 / (den * both)
    term = pbe_gamma * jnp.log(both * both * inv)
    term_t = pbe_beta * (y1 + y) * inv
    term_c = (-pbe_beta / pbe_gamma) * (t_square * t_square) * (y * (1.0 + y1)) * inv * (factor * grown * inv_e)

    per_cell = exch * enhance + corr + term
    d_dens = (
        per_cell
        + (1.0 / 3.0) * exch * enhance
        - (8.0 / 3.0) * exch_slope * s_square
        - (1.0 / 3.0) * corr_rs * (1.0 + term_c)
        - (7.0 / 3.0) * term_t * t_square
    )
    twice_d_grad = (2.0 * n) * (exch_slope * s_n + term_t * t_n)
    return n * per_cell, d_dens, twice_d_grad


def block_turn(parts):
    group = lax.broadcasted_iota(jnp.int32, parts[0].shape, 1) // 32
    turned = [parts[0]] + [pltpu.roll(parts[b], 32 * b, 1) for b in range(1, 4)]
    out = []
    for a in range(4):
        mixed = jnp.where(
            group < 2,
            jnp.where(group == 0, turned[-a % 4], turned[(1 - a) % 4]),
            jnp.where(group == 2, turned[(2 - a) % 4], turned[(3 - a) % 4]),
        )
        out.append(mixed if a == 0 else pltpu.roll(mixed, 128 - 32 * a, 1))
    return out


FAR_FIRST = (2, 1, 3, 0)
CHUNKS = 8


def kernel(
    f_hbm, mats_hbm, out_ref, en_ref,
    f_ref, mats,
    send_n, send_g, got_n, got_g, plane_n, plane_x, plane_y, plane_d,
    send_f, send_v, got_f, got_v, div_z, e_own, e_row, e_mid, e_all,
    load_sem, send_sem, recv_sem, chunk_sem, planes_sem,
):
    j = lax.axis_index("gx")
    k = lax.axis_index("gy")
    me = j * NK + k
    own = pl.ds(pl.multiple_of(me * 8, 8), 8)
    chip_z, core, chip_x = j >> 2, j & 1, k & 3
    chip_y = (j & 2) + (k >> 2)
    at_z = [((chip_z + d) & 3) << 5 for d in range(4)]
    at_x = [(chip_x + d) & 3 for d in range(4)]

    def at_y(d):
        y = (chip_y + d) & 3
        return ((y & 2) << 3) + ((y & 1) << 2)

    load_f = pltpu.make_async_copy(f_hbm, f_ref, load_sem.at[0])
    load_m = pltpu.make_async_copy(mats_hbm, mats, load_sem.at[1])
    load_f.start()
    load_m.start()

    all_y = [at_y(d) for d in range(4)]
    cores = [core << 3, (1 - core) << 3]
    steps = [(dz, dy, dx, dc) for dz in range(4) for dy in range(4) for dx in range(4) for dc in range(2)][1:]
    steps = sorted(steps, key=lambda s: (-sum(min(d, 4 - d) for d in s[:3]), s))
    near = [s for s in steps if 0 in s[:3]]
    far = [s for s in steps if 0 not in s[:3]]

    def at_step(s):
        return at_z[s[0]] + all_y[s[1]] + cores[s[3]] + at_x[s[2]]

    barrier = pltpu.get_barrier_semaphore()
    with jax.named_scope("greet"):
        for s in near:
            pl.semaphore_signal(barrier, inc=1, device_id=at_step(s), device_id_type=LOGICAL)

    def chunk_at(i, sign):
        turn = i + 1
        side = (core ^ ((turn >> 2) & 1)) << 3
        return [(d, at_z[sign * d % 4] + at_y(sign * (d + turn)) + side) for d in FAR_FIRST]

    def send_chunk(i, sign, last, one):
        for d, base in chunk_at(i, sign):
            for dx in FAR_FIRST:
                if not (last and d == 0 and dx == 0):
                    one(base + at_x[dx])

    def send_to(p, src, dst, s, r):
        pltpu.make_async_remote_copy(
            src_ref=src, dst_ref=dst, send_sem=send_sem.at[s], recv_sem=r, device_id=p, device_id_type=LOGICAL
        ).start()

    def piece(ref, p):
        return ref.at[pl.ds(pl.multiple_of(p * 8, 8), 8)]

    def send_all_chunks(src, dst, s, sem_of, sign):
        def chunk(i, carry):
            send_chunk(i, sign, False, lambda p: send_to(p, piece(src, p), dst.at[own], s, sem_of(i)))
            return carry

        lax.fori_loop(0, CHUNKS - 1, chunk, 0)
        i = CHUNKS - 1
        send_chunk(i, sign, True, lambda p: send_to(p, piece(src, p), dst.at[own], s, sem_of(i)))
        dst[own, :] = src[own, :]

    def wait_all(ref, sem, rows):
        part = ref.at[pl.ds(0, rows)]
        pltpu.make_async_copy(part, part, sem).wait()

    def lay_out(ref, h, block):
        for c in range(2):
            for zz in range(2):
                ref[pl.ds(2 * (2 * h + c) + zz, 128, stride=8), :] = block[
                    128 * zz : 128 * zz + 128, 128 * c : 128 * c + 128
                ]

    with jax.named_scope("load"):
        load_f.wait()
        turned = [f_ref[256 * h : 256 * h + 256, :].T for h in range(2)]
        for h in range(2):
            lay_out(send_n, h, turned[h])
    def send_n_to(some):
        for s in some:
            p = at_step(s)
            send_to(p, piece(send_n, p), got_n.at[own], 0, recv_sem.at[0])

    with jax.named_scope("barrier"):
        pl.semaphore_wait(barrier, len(near))
        for dz in (2, 1, 3):
            pl.semaphore_signal(planes_sem, inc=1, device_id=at_step((dz, 0, 0, 0)), device_id_type=LOGICAL)
    with jax.named_scope("send_n"):
        send_n_to(near)
        got_n[own, :] = send_n[own, :]
    with jax.named_scope("barrier_far"):
        pl.semaphore_wait(planes_sem, 3)
    with jax.named_scope("send_n_far"):
        send_n_to(far)
    with jax.named_scope("grad_z"):
        load_m.wait()
        deriv = (mats[0], mats[1])
        deriv_x = (mats[2], mats[3])
        for h in range(2):
            lay_out(send_g, h, matmul(deriv, split(turned[h])))
    with jax.named_scope("send_g"):
        send_all_chunks(send_g, got_g, 1, lambda i: chunk_sem.at[i], 1)

    moved = 8 * (ND - 1)
    with jax.named_scope("wait_n"):
        wait_all(got_n, recv_sem.at[0], moved)

    def quad(ref, jk):
        return block_turn([ref[pl.ds(pl.multiple_of(jk * 32 + 8 * k4, 8), 8), :] for k4 in range(4)])

    def plane_of(ref, zz):
        return jnp.concatenate([ref[kh, pl.ds(zz, N, stride=2), :] for kh in range(2)], axis=1)

    with jax.named_scope("grad_xy"):
        for jk in range(2 * NJ):
            for x4, part in enumerate(quad(got_n, jk)):
                plane_n[jk % 2, 128 * x4 + 8 * (jk // 2) : 128 * x4 + 8 * (jk // 2) + 8, :] = part
        for zz in range(2):
            field = split(plane_of(plane_n, zz))
            along_x = matmul(deriv_x, field)
            along_y = matmul(field, deriv)
            for kh in range(2):
                plane_x[kh, pl.ds(zz, N, stride=2), :] = along_x[:, 128 * kh : 128 * kh + 128]
                plane_y[kh, pl.ds(zz, N, stride=2), :] = -along_y[:, 128 * kh : 128 * kh + 128]

    def cells(i, total, last):
        wait_all(got_g, chunk_sem.at[i], 120 if last else 128)
        quads = [base >> 2 for _, base in chunk_at(i, -1)]
        for group in (quads[:2], quads[2:]):
            refs = [
                (jk & 1, pl.ds(pl.multiple_of(128 * x4 + (jk >> 1) * 8, 8), 8), slice(None))
                for jk in group
                for x4 in range(4)
            ]
            n = jnp.concatenate([plane_n[r] for r in refs], axis=0)
            gx = jnp.concatenate([plane_x[r] for r in refs], axis=0)
            gy = jnp.concatenate([plane_y[r] for r in refs], axis=0)
            gz = jnp.concatenate([part for jk in group for part in quad(got_g, jk)], axis=0)
            f, d_dens, slope = xc_parts(n, gx * gx + gy * gy + gz * gz)
            fx, fy, fz = slope * gx, slope * gy, slope * gz
            for g, jk in enumerate(group):
                parts = block_turn([fz[32 * g + 8 * x4 : 32 * g + 8 * x4 + 8] for x4 in range(4)])
                for k4, part in enumerate(parts):
                    send_f[pl.ds(pl.multiple_of(jk * 32 + 8 * k4, 8), 8), :] = part
            for i8, r in enumerate(refs):
                plane_d[r] = d_dens[8 * i8 : 8 * i8 + 8]
                plane_x[r] = fx[8 * i8 : 8 * i8 + 8]
                plane_y[r] = fy[8 * i8 : 8 * i8 + 8]
                total = total + f[8 * i8 : 8 * i8 + 8]
        send_chunk(i, -1, last, lambda p: send_to(p, piece(send_f, p), got_f.at[own], 2, recv_sem.at[2]))
        return total

    with jax.named_scope("cells"):
        total = lax.fori_loop(0, CHUNKS - 1, functools.partial(cells, last=False), jnp.zeros((8, 128), F32))
        total = cells(CHUNKS - 1, total, last=True)
        mine = jnp.sum(total, axis=0, keepdims=True)
        e_own[0] = mine
        e_row[k] = mine
        got_f[own, :] = send_f[own, :]

    def send_row(i, carry):
        send_to(j * NK + ((k + i) & (NK - 1)), e_own.at[0], e_row.at[k], 4, recv_sem.at[4])
        return carry

    lax.fori_loop(1, NK, send_row, 0)

    with jax.named_scope("divergence"):
        for zz in range(2):
            along = matmul(deriv_x, split(plane_of(plane_x, zz))) - matmul(split(plane_of(plane_y, zz)), deriv)
            for kh in range(2):
                rows = (kh, pl.ds(zz, N, stride=2), slice(None))
                plane_d[rows] = plane_d[rows] - along[:, 128 * kh : 128 * kh + 128]
        for jk in range(2 * NJ):
            parts = block_turn(
                [plane_d[jk % 2, 128 * x4 + 8 * (jk // 2) : 128 * x4 + 8 * (jk // 2) + 8, :] for x4 in range(4)]
            )
            for k4, part in enumerate(parts):
                send_v[jk * 32 + 8 * k4 : jk * 32 + 8 * k4 + 8, :] = part

    with jax.named_scope("send_v"):
        send_all_chunks(send_v, got_v, 3, lambda i: recv_sem.at[3], -1)

    with jax.named_scope("energy_row"):
        wait_all(e_row, recv_sem.at[4], NK - 1)
        row = jnp.sum(e_row[...], axis=0)
        e_mid[0] = row
        e_all[j] = row

        def send_col(i, carry):
            send_to(((j + i) & (NJ - 1)) * NK + k, e_mid.at[0], e_all.at[j], 5, recv_sem.at[5])
            return carry

        lax.fori_loop(1, NJ, send_col, 0)

    def gathered(ref, h):
        return jnp.concatenate(
            [
                jnp.concatenate([ref[pl.ds(2 * (2 * h + c) + zz, 128, stride=8), :] for c in range(2)], axis=1)
                for zz in range(2)
            ],
            axis=0,
        )

    with jax.named_scope("wait_f"):
        wait_all(got_f, recv_sem.at[2], moved)
    with jax.named_scope("div_z"):
        for h in range(2):
            div_z[h] = matmul(deriv, split(gathered(got_f, h)))
    with jax.named_scope("wait_v"):
        wait_all(got_v, recv_sem.at[3], moved)
    with jax.named_scope("finish"):
        for h in range(2):
            out_ref[256 * h : 256 * h + 256, :] = (gathered(got_v, h) - div_z[h]).T

    with jax.named_scope("energy"):
        wait_all(e_all, recv_sem.at[5], NJ - 1)
        en_ref[0, 0] = jnp.sum(jnp.sum(e_all[...], axis=0)) * (1.0 / N**3)
        for s, ref in enumerate((send_n, send_g, send_f, send_v)):
            wait_all(ref, send_sem.at[s], moved)
        wait_all(e_row, send_sem.at[4], NK - 1)
        wait_all(e_all, send_sem.at[5], NJ - 1)


def body(density):
    flat = density.reshape(-1, density.shape[2])
    deriv = deriv_matrix()
    order = row_order()
    mats = np.stack(split_np(deriv) + split_np(deriv[order][:, order]))
    hbm = pl.BlockSpec(memory_space=pltpu.HBM)
    lines = pltpu.VMEM((ROWS, 128), F32)
    planes = pltpu.VMEM((2, 2 * N, 128), F32)
    potential, energy = pl.pallas_call(
        kernel,
        name="pbe",
        out_shape=(
            jax.ShapeDtypeStruct(flat.shape, F32),
            jax.ShapeDtypeStruct((1, 1), F32),
        ),
        in_specs=[hbm] * 2,
        out_specs=(pl.BlockSpec(memory_space=pltpu.VMEM), pl.BlockSpec(memory_space=pltpu.SMEM)),
        scratch_shapes=[pltpu.VMEM(flat.shape, F32), pltpu.VMEM((4, N, N), BF16)]
        + [lines] * 4
        + [planes] * 4
        + [lines] * 4
        + [
            pltpu.VMEM((2, N, N), F32),
            pltpu.VMEM((1, 1, 128), F32),
            pltpu.VMEM((NK, 1, 128), F32),
            pltpu.VMEM((1, 1, 128), F32),
            pltpu.VMEM((NJ, 1, 128), F32),
            pltpu.SemaphoreType.DMA((2,)),
            pltpu.SemaphoreType.DMA((6,)),
            pltpu.SemaphoreType.DMA((6,)),
            pltpu.SemaphoreType.DMA((NJ // 2,)),
            pltpu.SemaphoreType.REGULAR,
        ],
        compiler_params=pltpu.CompilerParams(collective_id=0, has_side_effects=True, vmem_limit_bytes=40 * 2**20),
    )(*(pltpu.with_memory_space_constraint(a, pltpu.HBM) for a in (flat, jnp.asarray(mats))))
    return potential.reshape(density.shape), energy[0, 0]


def solution(mesh):
    return jax.shard_map(
        body,
        mesh=mesh,
        in_specs=(P("gx", "gy", None),),
        out_specs=(P("gx", "gy", None), P()),
        check_vma=False,
    )
```

```python
import functools
import math

import jax
import jax.numpy as jnp
import numpy as np
from jax import lax
from jax.experimental import pallas as pl
from jax.experimental.pallas import tpu as pltpu
from jax.sharding import PartitionSpec as P

LOGICAL = pl.DeviceIdType.LOGICAL
F32 = jnp.float32
BF16 = jnp.bfloat16

N = 256
NJ = 16
NK = 8
ND = NJ * NK
ROWS = N * N * N // ND // 128

pbe_kappa = 0.804
pbe_mu = 0.2195149727645171
pbe_beta = 0.06672455060314922
pbe_gamma = 0.031090690869654894
pw_coef = 0.0310907
pw_alpha = 0.2137
pw_first = 7.5957
pw_second = 3.5876
pw_third = 1.6382
pw_fourth = 0.49294

kf_coef = (3.0 * math.pi**2) ** (1.0 / 3.0)
rs_coef = (3.0 / (4.0 * math.pi)) ** (1.0 / 3.0)


def deriv_matrix():
    m = np.arange(N)
    signed = np.where(m < N // 2, m, m - N)
    signed = np.where(m == N // 2, 0, signed) * (2.0 * math.pi / N)
    shift = (m[:, None] - m[None, :]) % N
    line = -(signed[None, :] * np.sin(2.0 * math.pi * (m[:, None] * m[None, :] % N) / N)).sum(1) / N
    return line[shift]


def row_order():
    r = np.arange(N)
    return 16 * (r // 16) + 4 * (r % 4) + (r // 4) % 4


def split_np(a):
    hi = a.astype(jnp.bfloat16)
    lo = (a - hi.astype(np.float64)).astype(jnp.bfloat16)
    return hi, lo


def split(a):
    hi = a.astype(BF16)
    lo = (a - hi.astype(F32)).astype(BF16)
    return hi, lo


def dot(a, b):
    return jnp.dot(a, b, preferred_element_type=F32)


def matmul(a, b):
    (ah, al), (bh, bl) = a, b
    return dot(ah, bh) + (dot(ah, bl) + dot(al, bh))


def xc_parts(n, g):
    w = jnp.exp2(jnp.log(n) * (-1.0 / (6.0 * math.log(2.0))))
    w2 = w * w
    w4 = w2 * w2
    w6 = w4 * w2
    w14 = (w4 * w4) * w6
    cube = n * w4
    g14 = g * w14
    both_t = g14 * (pbe_beta / pbe_gamma * math.pi / (16.0 * kf_coef))
    s_scaled = (g14 * w2) * (pbe_mu / pbe_kappa / (4.0 * kf_coef**2))
    quot = 1.0 / (1.0 + s_scaled)
    c_x = -0.75 * kf_coef / math.pi
    cube_quot = cube * quot
    exch = cube * (c_x * (1.0 + pbe_kappa)) - cube_quot * (c_x * pbe_kappa)
    cube_quot2 = cube_quot * quot

    c2 = 2.0 * pw_coef
    r1 = math.sqrt(rs_coef)
    a1, a2, a3, a4 = c2 * pw_first * r1, c2 * pw_second * r1**2, c2 * pw_third * r1**3, c2 * pw_fourth * r1**4
    series = w * (a1 + w * (a2 + w * (a3 + w * a4)))
    series_rs = w * (0.5 * a1 + w * (a2 + w * (1.5 * a3 + w * (2.0 * a4))))
    series1 = series + 1.0
    inv_both = 1.0 / (series * series1)
    logarithm = jnp.log(1.0 + series1 * inv_both)
    alpha = w2 * (c2 * pw_alpha * rs_coef)
    lead = c2 + alpha
    minus_corr = lead * logarithm
    corr_rs = lead * (series_rs * inv_both) - alpha * logarithm

    grown = jnp.exp2(minus_corr * (1.0 / (pbe_gamma * math.log(2.0))))
    inv_e = 1.0 / (grown - 1.0)
    y = inv_e * both_t
    y1 = 1.0 + y
    yy = y * y
    den = y1 + yy
    both = den + both_t * y1
    inv = 1.0 / (den * both)
    term = pbe_gamma * jnp.log(both * both * inv)
    slope_t = (y1 + y) * inv
    term_t = (both_t * slope_t) * (-7.0 / 3.0 * pbe_gamma)
    term_c = ((yy * both_t) * (1.0 + y1)) * ((inv * inv_e) * grown)

    per_cell = (exch - minus_corr) + term
    exch_s = (cube_quot2 * s_scaled) * (-8.0 / 3.0 * c_x * pbe_kappa)
    d_dens = per_cell + (exch - corr_rs * (1.0 - term_c)) * (1.0 / 3.0) + (exch_s + term_t)
    twice_d_grad = (n * w14) * (
        (cube_quot2 * w2) * (2.0 * c_x * pbe_mu / (4.0 * kf_coef**2))
        + slope_t * (2.0 * pbe_beta * math.pi / (16.0 * kf_coef))
    )
    return n * per_cell, d_dens, twice_d_grad


def block_turn(parts):
    group = lax.broadcasted_iota(jnp.int32, parts[0].shape, 1) // 32
    turned = [parts[0]] + [pltpu.roll(parts[b], 32 * b, 1) for b in range(1, 4)]
    out = []
    for a in range(4):
        mixed = jnp.where(
            group < 2,
            jnp.where(group == 0, turned[-a % 4], turned[(1 - a) % 4]),
            jnp.where(group == 2, turned[(2 - a) % 4], turned[(3 - a) % 4]),
        )
        out.append(mixed if a == 0 else pltpu.roll(mixed, 128 - 32 * a, 1))
    return out


FAR_FIRST = (2, 1, 3, 0)
CHUNKS = 8
GROUPS = ((0, 1), (2, 3))


def kernel(
    f_hbm, mats_hbm, out_ref, en_ref,
    f_ref, mats,
    send_n, send_g, got_n, got_g, plane_n, plane_x, plane_y, plane_d,
    send_f, send_v, got_f, got_v, div_z, e_own, e_row, e_mid, e_all,
    load_sem, send_sem, recv_sem, chunk_sem, planes_sem,
):
    j = lax.axis_index("gx")
    k = lax.axis_index("gy")
    me = j * NK + k
    own = pl.ds(pl.multiple_of(me * 8, 8), 8)
    chip_z, core, chip_x = j >> 2, j & 1, k & 3
    chip_y = (j & 2) + (k >> 2)
    at_z = [((chip_z + d) & 3) << 5 for d in range(4)]
    at_x = [(chip_x + d) & 3 for d in range(4)]

    def at_y(d):
        y = (chip_y + d) & 3
        return ((y & 2) << 3) + ((y & 1) << 2)

    load_f = pltpu.make_async_copy(f_hbm, f_ref, load_sem.at[0])
    load_m = pltpu.make_async_copy(mats_hbm, mats, load_sem.at[1])
    all_y = [at_y(d) for d in range(4)]
    cores = [core << 3, (1 - core) << 3]
    steps = [(dz, dy, dx, dc) for dz in range(4) for dy in range(4) for dx in range(4) for dc in range(2)][1:]
    steps = sorted(steps, key=lambda s: (-sum(min(d, 4 - d) for d in s[:3]), s))
    near = [s for s in steps if 0 in s[:3]]
    far = [s for s in steps if 0 not in s[:3]]

    def at_step(s):
        return at_z[s[0]] + all_y[s[1]] + cores[s[3]] + at_x[s[2]]

    barrier = pltpu.get_barrier_semaphore()
    with jax.named_scope("greet"):
        for s in near:
            pl.semaphore_signal(barrier, inc=1, device_id=at_step(s), device_id_type=LOGICAL)
        load_f.start()
        load_m.start()

    def chunk_at(i, sign):
        turn = i + 1
        side = (core ^ ((turn >> 2) & 1)) << 3
        return [(d, at_z[sign * d % 4] + at_y(sign * (d + turn)) + side) for d in FAR_FIRST]

    def send_chunk(i, sign, last, one):
        for d, base in chunk_at(i, sign):
            for dx in FAR_FIRST:
                if not (last and d == 0 and dx == 0):
                    one(base + at_x[dx])

    def send_to(p, src, dst, s, r):
        pltpu.make_async_remote_copy(
            src_ref=src, dst_ref=dst, send_sem=send_sem.at[s], recv_sem=r, device_id=p, device_id_type=LOGICAL
        ).start()

    def piece(ref, p):
        return ref.at[pl.ds(pl.multiple_of(p * 8, 8), 8)]

    def send_all_chunks(src, dst, s, sem_of, sign):
        def chunk(i, carry):
            send_chunk(i, sign, False, lambda p: send_to(p, piece(src, p), dst.at[own], s, sem_of(i)))
            return carry

        lax.fori_loop(0, CHUNKS - 1, chunk, 0)
        i = CHUNKS - 1
        send_chunk(i, sign, True, lambda p: send_to(p, piece(src, p), dst.at[own], s, sem_of(i)))
        dst[own, :] = src[own, :]

    def wait_all(ref, sem, rows):
        part = ref.at[pl.ds(0, rows)]
        pltpu.make_async_copy(part, part, sem).wait()

    def lay_out(ref, h, block):
        for c in range(2):
            for zz in range(2):
                ref[pl.ds(2 * (2 * h + c) + zz, 128, stride=8), :] = block[
                    128 * zz : 128 * zz + 128, 128 * c : 128 * c + 128
                ]

    with jax.named_scope("load"):
        load_f.wait()
        turned = [f_ref[256 * h : 256 * h + 256, :].T for h in range(2)]
        for h in range(2):
            lay_out(send_n, h, turned[h])
    def send_n_to(some):
        for s in some:
            p = at_step(s)
            send_to(p, piece(send_n, p), got_n.at[own], 0, recv_sem.at[0])

    with jax.named_scope("barrier"):
        pl.semaphore_wait(barrier, len(near))
        for dz in (2, 1, 3):
            pl.semaphore_signal(planes_sem, inc=1, device_id=at_step((dz, 0, 0, 0)), device_id_type=LOGICAL)
    with jax.named_scope("send_n"):
        send_n_to(near)
        got_n[own, :] = send_n[own, :]
    with jax.named_scope("barrier_far"):
        pl.semaphore_wait(planes_sem, 3)
    with jax.named_scope("send_n_far"):
        send_n_to(far)
    with jax.named_scope("grad_z"):
        load_m.wait()
        deriv = (mats[0], mats[1])
        deriv_x = (mats[2], mats[3])
        for h in range(2):
            lay_out(send_g, h, matmul(deriv, split(turned[h])))
    with jax.named_scope("send_g"):
        send_all_chunks(send_g, got_g, 1, lambda i: chunk_sem.at[i], 1)

    moved = 8 * (ND - 1)
    with jax.named_scope("wait_n"):
        wait_all(got_n, recv_sem.at[0], moved)

    def turn_quad(block):
        return jnp.concatenate(block_turn([block[8 * b : 8 * b + 8] for b in range(4)]), axis=0)

    def lines_at(jk):
        return pl.ds(pl.multiple_of(jk * 32, 32), 32)

    def plane_of(ref, zz):
        return jnp.concatenate([ref[kh, pl.ds(zz, N, stride=2), :] for kh in range(2)], axis=1)

    with jax.named_scope("grad_xy"):
        for jk in range(2 * NJ):
            plane_n[jk % 2, 32 * (jk // 2) : 32 * (jk // 2) + 32, :] = turn_quad(got_n[32 * jk : 32 * jk + 32, :])
        for zz in range(2):
            field = split(plane_of(plane_n, zz))
            along_x = matmul(deriv_x, field)
            along_y = matmul(field, deriv)
            for kh in range(2):
                plane_x[kh, pl.ds(zz, N, stride=2), :] = along_x[:, 128 * kh : 128 * kh + 128]
                plane_y[kh, pl.ds(zz, N, stride=2), :] = -along_y[:, 128 * kh : 128 * kh + 128]

    def cells(i, total, last):
        wait_all(got_g, chunk_sem.at[i], 120 if last else 128)
        quads = [base >> 2 for _, base in chunk_at(i, -1)]
        for group in GROUPS:
            group = [quads[q] for q in group]
            refs = [(jk & 1, lines_at(jk >> 1), slice(None)) for jk in group]
            n = jnp.concatenate([plane_n[r] for r in refs], axis=0)
            gx = jnp.concatenate([plane_x[r] for r in refs], axis=0)
            gy = jnp.concatenate([plane_y[r] for r in refs], axis=0)
            gz = jnp.concatenate([turn_quad(got_g[lines_at(jk), :]) for jk in group], axis=0)
            f, d_dens, slope = xc_parts(n, gx * gx + gy * gy + gz * gz)
            fx, fy, fz = slope * gx, slope * gy, slope * gz
            for g, jk in enumerate(group):
                send_f[lines_at(jk), :] = turn_quad(fz[32 * g : 32 * g + 32])
            for g, r in enumerate(refs):
                plane_d[r] = d_dens[32 * g : 32 * g + 32]
                plane_x[r] = fx[32 * g : 32 * g + 32]
                plane_y[r] = fy[32 * g : 32 * g + 32]
            for i8 in range(4 * len(group)):
                total = total + f[8 * i8 : 8 * i8 + 8]
        send_chunk(i, -1, last, lambda p: send_to(p, piece(send_f, p), got_f.at[own], 2, recv_sem.at[2]))
        return total

    with jax.named_scope("cells"):
        total = lax.fori_loop(0, CHUNKS - 1, functools.partial(cells, last=False), jnp.zeros((8, 128), F32))
        total = cells(CHUNKS - 1, total, last=True)
        mine = jnp.sum(total, axis=0, keepdims=True)
        e_own[0] = mine
        e_row[k] = mine
        got_f[own, :] = send_f[own, :]

    def send_row(i, carry):
        send_to(j * NK + ((k + i) & (NK - 1)), e_own.at[0], e_row.at[k], 4, recv_sem.at[4])
        return carry

    lax.fori_loop(1, NK, send_row, 0)

    with jax.named_scope("divergence"):
        for zz in range(2):
            along = matmul(deriv_x, split(plane_of(plane_x, zz))) - matmul(split(plane_of(plane_y, zz)), deriv)
            for kh in range(2):
                rows = (kh, pl.ds(zz, N, stride=2), slice(None))
                plane_d[rows] = plane_d[rows] - along[:, 128 * kh : 128 * kh + 128]
        for jk in range(2 * NJ):
            send_v[32 * jk : 32 * jk + 32, :] = turn_quad(plane_d[jk % 2, 32 * (jk // 2) : 32 * (jk // 2) + 32, :])

    def v_chunk(i, last=False):
        send_chunk(i, -1, last, lambda p: send_to(p, piece(send_v, p), got_v.at[own], 3, recv_sem.at[3]))

    def v_loop(i, carry):
        v_chunk(i)
        return carry

    with jax.named_scope("send_v"):
        lax.fori_loop(0, CHUNKS - 2, v_loop, 0)
        got_v[own, :] = send_v[own, :]

    with jax.named_scope("energy_row"):
        wait_all(e_row, recv_sem.at[4], NK - 1)
        row = jnp.sum(e_row[...], axis=0)
        e_mid[0] = row
        e_all[j] = row

        def send_col(i, carry):
            send_to(((j + i) & (NJ - 1)) * NK + k, e_mid.at[0], e_all.at[j], 5, recv_sem.at[5])
            return carry

        lax.fori_loop(1, NJ, send_col, 0)

    with jax.named_scope("send_v_end"):
        v_chunk(CHUNKS - 2)
        v_chunk(CHUNKS - 1, last=True)

    def gathered(ref, h):
        return jnp.concatenate(
            [
                jnp.concatenate([ref[pl.ds(2 * (2 * h + c) + zz, 128, stride=8), :] for c in range(2)], axis=1)
                for zz in range(2)
            ],
            axis=0,
        )

    with jax.named_scope("wait_f"):
        wait_all(got_f, recv_sem.at[2], moved)
    with jax.named_scope("div_z"):
        for h in range(2):
            div_z[h] = matmul(deriv, split(gathered(got_f, h)))
    with jax.named_scope("energy"):
        wait_all(e_all, recv_sem.at[5], NJ - 1)
        en_ref[...] = jnp.full((8, 128), jnp.sum(jnp.sum(e_all[...], axis=0)) * (1.0 / N**3), F32)
    with jax.named_scope("sent"):
        for s, ref in enumerate((send_n, send_g, send_f)):
            wait_all(ref, send_sem.at[s], moved)
        wait_all(e_row, send_sem.at[4], NK - 1)
        wait_all(e_all, send_sem.at[5], NJ - 1)
    with jax.named_scope("wait_v"):
        wait_all(got_v, recv_sem.at[3], moved)
    with jax.named_scope("finish"):
        for h in range(2):
            out_ref[256 * h : 256 * h + 256, :] = (gathered(got_v, h) - div_z[h]).T

    wait_all(send_v, send_sem.at[3], moved)


def body(density):
    flat = density.reshape(-1, density.shape[2])
    deriv = deriv_matrix()
    order = row_order()
    mats = np.stack(split_np(deriv) + split_np(deriv[order][:, order]))
    hbm = pl.BlockSpec(memory_space=pltpu.HBM)
    lines = pltpu.VMEM((ROWS, 128), F32)
    planes = pltpu.VMEM((2, 2 * N, 128), F32)
    potential, energy = pl.pallas_call(
        kernel,
        name="pbe",
        out_shape=(
            jax.ShapeDtypeStruct(flat.shape, F32),
            jax.ShapeDtypeStruct((8, 128), F32),
        ),
        in_specs=[hbm] * 2,
        out_specs=(pl.BlockSpec(memory_space=pltpu.VMEM), pl.BlockSpec(memory_space=pltpu.VMEM)),
        scratch_shapes=[pltpu.VMEM(flat.shape, F32), pltpu.VMEM((4, N, N), BF16)]
        + [lines] * 4
        + [planes] * 4
        + [lines] * 4
        + [
            pltpu.VMEM((2, N, N), F32),
            pltpu.VMEM((1, 1, 128), F32),
            pltpu.VMEM((NK, 1, 128), F32),
            pltpu.VMEM((1, 1, 128), F32),
            pltpu.VMEM((NJ, 1, 128), F32),
            pltpu.SemaphoreType.DMA((2,)),
            pltpu.SemaphoreType.DMA((6,)),
            pltpu.SemaphoreType.DMA((6,)),
            pltpu.SemaphoreType.DMA((NJ // 2,)),
            pltpu.SemaphoreType.REGULAR,
        ],
        compiler_params=pltpu.CompilerParams(collective_id=0, has_side_effects=True, vmem_limit_bytes=40 * 2**20),
    )(*(pltpu.with_memory_space_constraint(a, pltpu.HBM) for a in (flat, jnp.asarray(mats))))
    return potential.reshape(density.shape), energy[0, 0]


def solution(mesh):
    return jax.shard_map(
        body,
        mesh=mesh,
        in_specs=(P("gx", "gy", None),),
        out_specs=(P("gx", "gy", None), P()),
        check_vma=False,
    )
```

```python
import functools
import math

import jax
import jax.numpy as jnp
import numpy as np
from jax import lax
from jax.experimental import pallas as pl
from jax.experimental.pallas import tpu as pltpu
from jax.sharding import PartitionSpec as P

LOGICAL = pl.DeviceIdType.LOGICAL
F32 = jnp.float32
BF16 = jnp.bfloat16

N = 256
NJ = 16
NK = 8
ND = NJ * NK
ROWS = N * N * N // ND // 128

pbe_kappa = 0.804
pbe_mu = 0.2195149727645171
pbe_beta = 0.06672455060314922
pbe_gamma = 0.031090690869654894
pw_coef = 0.0310907
pw_alpha = 0.2137
pw_first = 7.5957
pw_second = 3.5876
pw_third = 1.6382
pw_fourth = 0.49294

kf_coef = (3.0 * math.pi**2) ** (1.0 / 3.0)
rs_coef = (3.0 / (4.0 * math.pi)) ** (1.0 / 3.0)


def deriv_matrix():
    m = np.arange(N)
    signed = np.where(m < N // 2, m, m - N)
    signed = np.where(m == N // 2, 0, signed) * (2.0 * math.pi / N)
    shift = (m[:, None] - m[None, :]) % N
    line = -(signed[None, :] * np.sin(2.0 * math.pi * (m[:, None] * m[None, :] % N) / N)).sum(1) / N
    return line[shift]


def row_order():
    r = np.arange(N)
    return 16 * (r // 16) + 4 * (r % 4) + (r // 4) % 4


def split_np(a):
    hi = a.astype(jnp.bfloat16)
    lo = (a - hi.astype(np.float64)).astype(jnp.bfloat16)
    return hi, lo


def split(a):
    hi = a.astype(BF16)
    lo = (a - hi.astype(F32)).astype(BF16)
    return hi, lo


def dot(a, b):
    return jnp.dot(a, b, preferred_element_type=F32)


def matmul(a, b):
    (ah, al), (bh, bl) = a, b
    return dot(ah, bh) + (dot(ah, bl) + dot(al, bh))


def xc_parts(n, g):
    w = jnp.exp(jnp.log(n) * (-1.0 / 6.0))
    w2 = w * w
    w4 = w2 * w2
    w6 = w4 * w2
    w14 = (w4 * w4) * w6
    cube = n * w4
    g14 = g * w14
    both_t = g14 * (pbe_beta / pbe_gamma * math.pi / (16.0 * kf_coef))
    s_scaled = (g14 * w2) * (pbe_mu / pbe_kappa / (4.0 * kf_coef**2))
    quot = 1.0 / (1.0 + s_scaled)
    c_x = -0.75 * kf_coef / math.pi
    cube_quot = cube * quot
    exch = cube * (c_x * (1.0 + pbe_kappa)) - cube_quot * (c_x * pbe_kappa)
    cube_quot2 = cube_quot * quot

    c2 = 2.0 * pw_coef
    r1 = math.sqrt(rs_coef)
    a1, a2, a3, a4 = c2 * pw_first * r1, c2 * pw_second * r1**2, c2 * pw_third * r1**3, c2 * pw_fourth * r1**4
    series = w * (a1 + w * (a2 + w * (a3 + w * a4)))
    series_rs = w * (0.5 * a1 + w * (a2 + w * (1.5 * a3 + w * (2.0 * a4))))
    series1 = series + 1.0
    inv_both = 1.0 / (series * series1)
    logarithm = jnp.log(1.0 + series1 * inv_both)
    alpha = w2 * (c2 * pw_alpha * rs_coef)
    lead = c2 + alpha
    minus_corr = lead * logarithm
    corr_rs = lead * (series_rs * inv_both) - alpha * logarithm

    grown = jnp.exp(minus_corr * (1.0 / pbe_gamma))
    inv_e = 1.0 / (grown - 1.0)
    y = inv_e * both_t
    y1 = 1.0 + y
    yy = y * y
    den = y1 + yy
    both = den + both_t * y1
    inv = 1.0 / (den * both)
    term = pbe_gamma * jnp.log(both * both * inv)
    slope_t = (y1 + y) * inv
    term_t = (both_t * slope_t) * (-7.0 / 3.0 * pbe_gamma)
    term_c = ((yy * both_t) * (1.0 + y1)) * ((inv * inv_e) * grown)

    per_cell = (exch - minus_corr) + term
    exch_s = (cube_quot2 * s_scaled) * (-8.0 / 3.0 * c_x * pbe_kappa)
    d_dens = per_cell + (exch - corr_rs * (1.0 - term_c)) * (1.0 / 3.0) + (exch_s + term_t)
    twice_d_grad = (n * w14) * (
        (cube_quot2 * w2) * (2.0 * c_x * pbe_mu / (4.0 * kf_coef**2))
        + slope_t * (2.0 * pbe_beta * math.pi / (16.0 * kf_coef))
    )
    return n * per_cell, d_dens, twice_d_grad


def block_turn(parts):
    group = lax.broadcasted_iota(jnp.int32, parts[0].shape, 1) // 32
    turned = [parts[0]] + [pltpu.roll(parts[b], 32 * b, 1) for b in range(1, 4)]
    out = []
    for a in range(4):
        mixed = jnp.where(
            group < 2,
            jnp.where(group == 0, turned[-a % 4], turned[(1 - a) % 4]),
            jnp.where(group == 2, turned[(2 - a) % 4], turned[(3 - a) % 4]),
        )
        out.append(mixed if a == 0 else pltpu.roll(mixed, 128 - 32 * a, 1))
    return out


FAR_FIRST = (2, 1, 3, 0)
CHUNKS = 8
GROUPS = ((0, 1), (2, 3))


def kernel(
    f_hbm, mats_hbm, out_ref, en_ref,
    f_ref, mats,
    send_n, send_g, got_n, got_g, plane_n, plane_x, plane_y, plane_d,
    send_f, send_v, got_f, got_v, div_z, e_own, e_row, e_mid, e_all, e_out,
    load_sem, send_sem, recv_sem, chunk_sem, planes_sem, half_sem,
):
    j = lax.axis_index("gx")
    k = lax.axis_index("gy")
    me = j * NK + k
    own = pl.ds(pl.multiple_of(me * 8, 8), 8)
    chip_z, core, chip_x = j >> 2, j & 1, k & 3
    chip_y = (j & 2) + (k >> 2)
    at_z = [((chip_z + d) & 3) << 5 for d in range(4)]
    at_x = [(chip_x + d) & 3 for d in range(4)]

    def at_y(d):
        y = (chip_y + d) & 3
        return ((y & 2) << 3) + ((y & 1) << 2)

    load_f = pltpu.make_async_copy(f_hbm, f_ref, load_sem.at[0])
    load_m = pltpu.make_async_copy(mats_hbm, mats, load_sem.at[1])
    all_y = [at_y(d) for d in range(4)]
    cores = [core << 3, (1 - core) << 3]
    steps = [(dz, dy, dx, dc) for dz in range(4) for dy in range(4) for dx in range(4) for dc in range(2)][1:]
    steps = sorted(steps, key=lambda s: (-sum(min(d, 4 - d) for d in s[:3]), s))
    near = [s for s in steps if 0 in s[:3]]
    far = [s for s in steps if 0 not in s[:3]]

    def at_step(s):
        return at_z[s[0]] + all_y[s[1]] + cores[s[3]] + at_x[s[2]]

    same = [s for s in near if s[3] == 0]
    other = [s for s in near if s[3] == 1]
    barrier = pltpu.get_barrier_semaphore()
    with jax.named_scope("greet"):
        for s in same + other[-1:]:
            pl.semaphore_signal(barrier, inc=1, device_id=at_step(s), device_id_type=LOGICAL)
        load_f.start()
        load_m.start()

    def chunk_at(i, sign):
        turn = i + 1
        side = (core ^ ((turn >> 2) & 1)) << 3
        return [(d, at_z[sign * d % 4] + at_y(sign * (d + turn)) + side) for d in FAR_FIRST]

    def send_chunk(i, sign, last, one):
        for d, base in chunk_at(i, sign):
            for dx in FAR_FIRST:
                if not (last and d == 0 and dx == 0):
                    one(base + at_x[dx])

    def send_to(p, src, dst, s, r):
        pltpu.make_async_remote_copy(
            src_ref=src, dst_ref=dst, send_sem=send_sem.at[s], recv_sem=r, device_id=p, device_id_type=LOGICAL
        ).start()

    def piece(ref, p):
        return ref.at[pl.ds(pl.multiple_of(p * 8, 8), 8)]

    def send_all_chunks(src, dst, s, sem_of, sign):
        def chunk(i, carry):
            send_chunk(i, sign, False, lambda p: send_to(p, piece(src, p), dst.at[own], s, sem_of(i)))
            return carry

        lax.fori_loop(0, CHUNKS - 1, chunk, 0)
        i = CHUNKS - 1
        send_chunk(i, sign, True, lambda p: send_to(p, piece(src, p), dst.at[own], s, sem_of(i)))
        dst[own, :] = src[own, :]

    def wait_all(ref, sem, rows):
        part = ref.at[pl.ds(0, rows)]
        pltpu.make_async_copy(part, part, sem).wait()

    def lay_out(ref, h, block):
        for c in range(2):
            for zz in range(2):
                ref[pl.ds(2 * (2 * h + c) + zz, 128, stride=8), :] = block[
                    128 * zz : 128 * zz + 128, 128 * c : 128 * c + 128
                ]

    with jax.named_scope("load"):
        load_f.wait()
        turned = [f_ref[256 * h : 256 * h + 256, :].T for h in range(2)]
        for h in range(2):
            lay_out(send_n, h, turned[h])
    def send_n_to(some):
        for s in some:
            p = at_step(s)
            send_to(p, piece(send_n, p), got_n.at[own], 0, recv_sem.at[0])

    with jax.named_scope("barrier"):
        pl.semaphore_wait(barrier, len(same) + 1)
        pl.semaphore_signal(half_sem, inc=1, device_id=at_step((0, 0, 0, 1)), device_id_type=LOGICAL)
    with jax.named_scope("send_n"):
        send_n_to(same)
    with jax.named_scope("barrier_half"):
        pl.semaphore_wait(half_sem, 1)
        for dz in (2, 1, 3):
            pl.semaphore_signal(planes_sem, inc=1, device_id=at_step((dz, 0, 0, 0)), device_id_type=LOGICAL)
    with jax.named_scope("send_n2"):
        send_n_to(other)
        got_n[own, :] = send_n[own, :]
    with jax.named_scope("grad_z"):
        load_m.wait()
        deriv = (mats[0], mats[1])
        deriv_x = (mats[2], mats[3])
        for h in range(2):
            lay_out(send_g, h, matmul(deriv, split(turned[h])))
    with jax.named_scope("barrier_far"):
        pl.semaphore_wait(planes_sem, 3)
    with jax.named_scope("send_n_far"):
        send_n_to(far)
    with jax.named_scope("send_g"):
        send_all_chunks(send_g, got_g, 1, lambda i: chunk_sem.at[i], 1)

    moved = 8 * (ND - 1)
    with jax.named_scope("wait_n"):
        wait_all(got_n, recv_sem.at[0], moved)

    def turn_quad(block):
        return jnp.concatenate(block_turn([block[8 * b : 8 * b + 8] for b in range(4)]), axis=0)

    def lines_at(jk):
        return pl.ds(pl.multiple_of(jk * 32, 32), 32)

    def plane_of(ref, zz):
        return jnp.concatenate([ref[kh, pl.ds(zz, N, stride=2), :] for kh in range(2)], axis=1)

    with jax.named_scope("grad_xy"):
        for jk in range(2 * NJ):
            plane_n[jk % 2, 32 * (jk // 2) : 32 * (jk // 2) + 32, :] = turn_quad(got_n[32 * jk : 32 * jk + 32, :])
        for zz in range(2):
            field = split(plane_of(plane_n, zz))
            along_x = matmul(deriv_x, field)
            along_y = matmul(field, deriv)
            for kh in range(2):
                plane_x[kh, pl.ds(zz, N, stride=2), :] = along_x[:, 128 * kh : 128 * kh + 128]
                plane_y[kh, pl.ds(zz, N, stride=2), :] = -along_y[:, 128 * kh : 128 * kh + 128]

    def cells(i, total, last):
        wait_all(got_g, chunk_sem.at[i], 120 if last else 128)
        quads = [base >> 2 for _, base in chunk_at(i, -1)]
        for group in GROUPS:
            group = [quads[q] for q in group]
            refs = [(jk & 1, lines_at(jk >> 1), slice(None)) for jk in group]
            n = jnp.concatenate([plane_n[r] for r in refs], axis=0)
            gx = jnp.concatenate([plane_x[r] for r in refs], axis=0)
            gy = jnp.concatenate([plane_y[r] for r in refs], axis=0)
            gz = jnp.concatenate([turn_quad(got_g[lines_at(jk), :]) for jk in group], axis=0)
            f, d_dens, slope = xc_parts(n, gx * gx + gy * gy + gz * gz)
            fx, fy, fz = slope * gx, slope * gy, slope * gz
            for g, jk in enumerate(group):
                send_f[lines_at(jk), :] = turn_quad(fz[32 * g : 32 * g + 32])
            for g, r in enumerate(refs):
                plane_d[r] = d_dens[32 * g : 32 * g + 32]
                plane_x[r] = fx[32 * g : 32 * g + 32]
                plane_y[r] = fy[32 * g : 32 * g + 32]
            for i8 in range(4 * len(group)):
                total = total + f[8 * i8 : 8 * i8 + 8]
        send_chunk(i, -1, last, lambda p: send_to(p, piece(send_f, p), got_f.at[own], 2, recv_sem.at[2]))
        return total

    with jax.named_scope("cells"):
        total = lax.fori_loop(0, CHUNKS - 1, functools.partial(cells, last=False), jnp.zeros((8, 128), F32))
        total = cells(CHUNKS - 1, total, last=True)
        mine = jnp.sum(total, axis=0, keepdims=True)
        e_own[0] = mine
        e_row[k] = mine
        got_f[own, :] = send_f[own, :]

    def send_row(i, carry):
        send_to(j * NK + ((k + i) & (NK - 1)), e_own.at[0], e_row.at[k], 4, recv_sem.at[4])
        return carry

    lax.fori_loop(1, NK, send_row, 0)

    with jax.named_scope("divergence"):
        for zz in range(2):
            along = matmul(deriv_x, split(plane_of(plane_x, zz))) - matmul(split(plane_of(plane_y, zz)), deriv)
            for kh in range(2):
                rows = (kh, pl.ds(zz, N, stride=2), slice(None))
                plane_d[rows] = plane_d[rows] - along[:, 128 * kh : 128 * kh + 128]
        for jk in range(2 * NJ):
            send_v[32 * jk : 32 * jk + 32, :] = turn_quad(plane_d[jk % 2, 32 * (jk // 2) : 32 * (jk // 2) + 32, :])

    def send_v_to(some):
        for step in some:
            p = at_step(step)
            send_to(p, piece(send_v, p), got_v.at[own], 3, recv_sem.at[3])

    with jax.named_scope("send_v"):
        send_v_to(steps[:95])
        got_v[own, :] = send_v[own, :]

    with jax.named_scope("energy_row"):
        wait_all(e_row, recv_sem.at[4], NK - 1)
        row = jnp.sum(e_row[...], axis=0)
        e_mid[0] = row
        e_all[j] = row

        def send_col(i, carry):
            send_to(((j + i) & (NJ - 1)) * NK + k, e_mid.at[0], e_all.at[j], 5, recv_sem.at[5])
            return carry

        lax.fori_loop(1, NJ, send_col, 0)

    with jax.named_scope("send_v_end"):
        send_v_to(steps[95:])

    def gathered(ref, h):
        return jnp.concatenate(
            [
                jnp.concatenate([ref[pl.ds(2 * (2 * h + c) + zz, 128, stride=8), :] for c in range(2)], axis=1)
                for zz in range(2)
            ],
            axis=0,
        )

    with jax.named_scope("wait_f"):
        wait_all(got_f, recv_sem.at[2], moved)
    with jax.named_scope("div_z"):
        for h in range(2):
            div_z[h] = matmul(deriv, split(gathered(got_f, h)))
    with jax.named_scope("energy"):
        wait_all(e_all, recv_sem.at[5], NJ - 1)
        e_out[...] = jnp.full((8, 128), jnp.sum(jnp.sum(e_all[...], axis=0)) * (1.0 / N**3), F32)
        save_e = pltpu.make_async_copy(e_out, en_ref, load_sem.at[2])
        save_e.start()
    with jax.named_scope("sent"):
        for s, ref in enumerate((send_n, send_g, send_f)):
            wait_all(ref, send_sem.at[s], moved)
        wait_all(e_row, send_sem.at[4], NK - 1)
        wait_all(e_all, send_sem.at[5], NJ - 1)
    with jax.named_scope("wait_v"):
        wait_all(got_v, recv_sem.at[3], moved)
    with jax.named_scope("finish"):
        for h in range(2):
            out_ref[256 * h : 256 * h + 256, :] = (gathered(got_v, h) - div_z[h]).T

    wait_all(send_v, send_sem.at[3], moved)
    save_e.wait()


def store(p_ref, e_ref, p_hbm, e_hbm, scalar, sem):
    put_p = pltpu.make_async_copy(p_ref, p_hbm, sem.at[0])
    put_p.start()
    scalar[0, 0] = e_ref[0, 0]
    put_e = pltpu.make_async_copy(scalar, e_hbm, sem.at[1])
    put_e.start()
    put_p.wait()
    put_e.wait()


def body(density):
    flat = density.reshape(-1, density.shape[2])
    deriv = deriv_matrix()
    order = row_order()
    mats = np.stack(split_np(deriv) + split_np(deriv[order][:, order]))
    hbm = pl.BlockSpec(memory_space=pltpu.HBM)
    lines = pltpu.VMEM((ROWS, 128), F32)
    planes = pltpu.VMEM((2, 2 * N, 128), F32)
    potential, energy = pl.pallas_call(
        kernel,
        name="pbe",
        out_shape=(
            jax.ShapeDtypeStruct(flat.shape, F32),
            jax.ShapeDtypeStruct((8, 128), F32),
        ),
        in_specs=[hbm] * 2,
        out_specs=(pl.BlockSpec(memory_space=pltpu.VMEM), hbm),
        scratch_shapes=[pltpu.VMEM(flat.shape, F32), pltpu.VMEM((4, N, N), BF16)]
        + [lines] * 4
        + [planes] * 4
        + [lines] * 4
        + [
            pltpu.VMEM((2, N, N), F32),
            pltpu.VMEM((1, 1, 128), F32),
            pltpu.VMEM((NK, 1, 128), F32),
            pltpu.VMEM((1, 1, 128), F32),
            pltpu.VMEM((NJ, 1, 128), F32),
            pltpu.VMEM((8, 128), F32),
            pltpu.SemaphoreType.DMA((3,)),
            pltpu.SemaphoreType.DMA((6,)),
            pltpu.SemaphoreType.DMA((6,)),
            pltpu.SemaphoreType.DMA((NJ // 2,)),
            pltpu.SemaphoreType.REGULAR,
            pltpu.SemaphoreType.REGULAR,
        ],
        compiler_params=pltpu.CompilerParams(collective_id=0, has_side_effects=True, vmem_limit_bytes=40 * 2**20),
    )(*(pltpu.with_memory_space_constraint(a, pltpu.HBM) for a in (flat, jnp.asarray(mats))))
    potential, energy = pl.pallas_call(
        store,
        name="store",
        out_shape=(jax.ShapeDtypeStruct(flat.shape, F32), jax.ShapeDtypeStruct((1, 1), F32)),
        in_specs=[pl.BlockSpec(memory_space=pltpu.VMEM)] * 2,
        out_specs=(pl.BlockSpec(memory_space=pl.ANY), pl.BlockSpec(memory_space=pl.ANY)),
        scratch_shapes=[pltpu.SMEM((1, 1), F32), pltpu.SemaphoreType.DMA((2,))],
        compiler_params=pltpu.CompilerParams(vmem_limit_bytes=4 * 2**20),
    )(potential, energy)
    return potential.reshape(density.shape), energy[0, 0]


def solution(mesh):
    return jax.shard_map(
        body,
        mesh=mesh,
        in_specs=(P("gx", "gy", None),),
        out_specs=(P("gx", "gy", None), P()),
        check_vma=False,
    )
```

```python
import functools
import math

import jax
import jax.numpy as jnp
import numpy as np
from jax import lax
from jax.experimental import pallas as pl
from jax.experimental.pallas import tpu as pltpu
from jax.sharding import PartitionSpec as P

LOGICAL = pl.DeviceIdType.LOGICAL
F32 = jnp.float32
BF16 = jnp.bfloat16

N = 256
NJ = 16
NK = 8
ND = NJ * NK
ROWS = N * N * N // ND // 128

pbe_kappa = 0.804
pbe_mu = 0.2195149727645171
pbe_beta = 0.06672455060314922
pbe_gamma = 0.031090690869654894
pw_coef = 0.0310907
pw_alpha = 0.2137
pw_first = 7.5957
pw_second = 3.5876
pw_third = 1.6382
pw_fourth = 0.49294

kf_coef = (3.0 * math.pi**2) ** (1.0 / 3.0)
rs_coef = (3.0 / (4.0 * math.pi)) ** (1.0 / 3.0)


def deriv_matrix():
    m = np.arange(N)
    signed = np.where(m < N // 2, m, m - N)
    signed = np.where(m == N // 2, 0, signed) * (2.0 * math.pi / N)
    shift = (m[:, None] - m[None, :]) % N
    line = -(signed[None, :] * np.sin(2.0 * math.pi * (m[:, None] * m[None, :] % N) / N)).sum(1) / N
    return line[shift]


def row_order():
    r = np.arange(N)
    return 16 * (r // 16) + 4 * (r % 4) + (r // 4) % 4


def split_np(a):
    hi = a.astype(jnp.bfloat16)
    lo = (a - hi.astype(np.float64)).astype(jnp.bfloat16)
    return hi, lo


def split(a):
    hi = a.astype(BF16)
    lo = (a - hi.astype(F32)).astype(BF16)
    return hi, lo


def dot(a, b):
    return jnp.dot(a, b, preferred_element_type=F32)


def matmul(a, b):
    (ah, al), (bh, bl) = a, b
    return dot(ah, bh) + (dot(ah, bl) + dot(al, bh))


def xc_parts(n, g):
    w = jnp.exp(jnp.log(n) * (-1.0 / 6.0))
    w2 = w * w
    w4 = w2 * w2
    w6 = w4 * w2
    w14 = (w4 * w4) * w6
    cube = n * w4
    g14 = g * w14
    both_t = g14 * (pbe_beta / pbe_gamma * math.pi / (16.0 * kf_coef))
    s_scaled = (g14 * w2) * (pbe_mu / pbe_kappa / (4.0 * kf_coef**2))
    quot = 1.0 / (1.0 + s_scaled)
    c_x = -0.75 * kf_coef / math.pi
    cube_quot = cube * quot
    exch = cube * (c_x * (1.0 + pbe_kappa)) - cube_quot * (c_x * pbe_kappa)
    cube_quot2 = cube_quot * quot

    c2 = 2.0 * pw_coef
    r1 = math.sqrt(rs_coef)
    a1, a2, a3, a4 = c2 * pw_first * r1, c2 * pw_second * r1**2, c2 * pw_third * r1**3, c2 * pw_fourth * r1**4
    series = w * (a1 + w * (a2 + w * (a3 + w * a4)))
    series_rs = w * (0.5 * a1 + w * (a2 + w * (1.5 * a3 + w * (2.0 * a4))))
    series1 = series + 1.0
    inv_both = 1.0 / (series * series1)
    logarithm = jnp.log(1.0 + series1 * inv_both)
    alpha = w2 * (c2 * pw_alpha * rs_coef)
    lead = c2 + alpha
    minus_corr = lead * logarithm
    corr_rs = lead * (series_rs * inv_both) - alpha * logarithm

    grown = jnp.exp(minus_corr * (1.0 / pbe_gamma))
    inv_e = 1.0 / (grown - 1.0)
    y = inv_e * both_t
    y1 = 1.0 + y
    yy = y * y
    den = y1 + yy
    both = den + both_t * y1
    inv = 1.0 / (den * both)
    term = pbe_gamma * jnp.log(both * both * inv)
    slope_t = (y1 + y) * inv
    term_t = (both_t * slope_t) * (-7.0 / 3.0 * pbe_gamma)
    term_c = ((yy * both_t) * (1.0 + y1)) * ((inv * inv_e) * grown)

    per_cell = (exch - minus_corr) + term
    exch_s = (cube_quot2 * s_scaled) * (-8.0 / 3.0 * c_x * pbe_kappa)
    d_dens = per_cell + (exch - corr_rs * (1.0 - term_c)) * (1.0 / 3.0) + (exch_s + term_t)
    twice_d_grad = (n * w14) * (
        (cube_quot2 * w2) * (2.0 * c_x * pbe_mu / (4.0 * kf_coef**2))
        + slope_t * (2.0 * pbe_beta * math.pi / (16.0 * kf_coef))
    )
    return n * per_cell, d_dens, twice_d_grad


def block_turn(parts):
    group = lax.broadcasted_iota(jnp.int32, parts[0].shape, 1) // 32
    turned = [parts[0]] + [pltpu.roll(parts[b], 32 * b, 1) for b in range(1, 4)]
    out = []
    for a in range(4):
        mixed = jnp.where(
            group < 2,
            jnp.where(group == 0, turned[-a % 4], turned[(1 - a) % 4]),
            jnp.where(group == 2, turned[(2 - a) % 4], turned[(3 - a) % 4]),
        )
        out.append(mixed if a == 0 else pltpu.roll(mixed, 128 - 32 * a, 1))
    return out


FAR_FIRST = (2, 1, 3, 0)
CHUNKS = 8
GROUPS = ((0, 1), (2, 3))


def kernel(
    f_hbm, mats_hbm, out_ref, en_ref,
    f_ref, mats,
    send_n, send_g, got_n, got_g, plane_n, plane_x, plane_y, plane_d,
    send_f, send_v, got_f, got_v, div_z, e_own, e_row, e_mid, e_all, e_out,
    load_sem, send_sem, recv_sem, chunk_sem, planes_sem, half_sem,
):
    j = lax.axis_index("gx")
    k = lax.axis_index("gy")
    me = j * NK + k
    own = pl.ds(pl.multiple_of(me * 8, 8), 8)
    chip_z, core, chip_x = j >> 2, j & 1, k & 3
    chip_y = (j & 2) + (k >> 2)
    at_z = [((chip_z + d) & 3) << 5 for d in range(4)]
    at_x = [(chip_x + d) & 3 for d in range(4)]

    def at_y(d):
        y = (chip_y + d) & 3
        return ((y & 2) << 3) + ((y & 1) << 2)

    load_f = pltpu.make_async_copy(f_hbm, f_ref, load_sem.at[0])
    load_m = pltpu.make_async_copy(mats_hbm, mats, load_sem.at[1])
    all_y = [at_y(d) for d in range(4)]
    cores = [core << 3, (1 - core) << 3]
    steps = [(dz, dy, dx, dc) for dz in range(4) for dy in range(4) for dx in range(4) for dc in range(2)][1:]
    steps = sorted(steps, key=lambda s: (-sum(min(d, 4 - d) for d in s[:3]), s))
    near = [s for s in steps if 0 in s[:3]]
    far = [s for s in steps if 0 not in s[:3]]

    def at_step(s):
        return at_z[s[0]] + all_y[s[1]] + cores[s[3]] + at_x[s[2]]

    same = [s for s in near if s[3] == 0]
    other = [s for s in near if s[3] == 1]
    barrier = pltpu.get_barrier_semaphore()
    with jax.named_scope("greet"):
        for s in same + other[-1:]:
            pl.semaphore_signal(barrier, inc=1, device_id=at_step(s), device_id_type=LOGICAL)
        load_f.start()
        load_m.start()

    def chunk_at(i, sign):
        turn = i + 1
        side = (core ^ ((turn >> 2) & 1)) << 3
        return [(d, at_z[sign * d % 4] + at_y(sign * (d + turn)) + side) for d in FAR_FIRST]

    def send_chunk(i, sign, last, one):
        for d, base in chunk_at(i, sign):
            for dx in FAR_FIRST:
                if not (last and d == 0 and dx == 0):
                    one(base + at_x[dx])

    def send_to(p, src, dst, s, r):
        pltpu.make_async_remote_copy(
            src_ref=src, dst_ref=dst, send_sem=send_sem.at[s], recv_sem=r, device_id=p, device_id_type=LOGICAL
        ).start()

    def piece(ref, p):
        return ref.at[pl.ds(pl.multiple_of(p * 8, 8), 8)]

    def send_all_chunks(src, dst, s, sem_of, sign):
        def chunk(i, carry):
            send_chunk(i, sign, False, lambda p: send_to(p, piece(src, p), dst.at[own], s, sem_of(i)))
            return carry

        lax.fori_loop(0, CHUNKS - 1, chunk, 0)
        i = CHUNKS - 1
        send_chunk(i, sign, True, lambda p: send_to(p, piece(src, p), dst.at[own], s, sem_of(i)))
        dst[own, :] = src[own, :]

    def wait_all(ref, sem, rows):
        part = ref.at[pl.ds(0, rows)]
        pltpu.make_async_copy(part, part, sem).wait()

    def lay_out(ref, h, block):
        for c in range(2):
            for zz in range(2):
                ref[pl.ds(2 * (2 * h + c) + zz, 128, stride=8), :] = block[
                    128 * zz : 128 * zz + 128, 128 * c : 128 * c + 128
                ]

    with jax.named_scope("load"):
        load_f.wait()
        turned = [f_ref[256 * h : 256 * h + 256, :].T for h in range(2)]
        for h in range(2):
            lay_out(send_n, h, turned[h])
    def send_n_to(some):
        for s in some:
            p = at_step(s)
            send_to(p, piece(send_n, p), got_n.at[own], 0, recv_sem.at[0])

    with jax.named_scope("barrier"):
        pl.semaphore_wait(barrier, len(same) + 1)
        pl.semaphore_signal(half_sem, inc=1, device_id=at_step((0, 0, 0, 1)), device_id_type=LOGICAL)
    with jax.named_scope("send_n"):
        send_n_to(same)
    with jax.named_scope("barrier_half"):
        pl.semaphore_wait(half_sem, 1)
        for dz in (2, 1, 3):
            pl.semaphore_signal(planes_sem, inc=1, device_id=at_step((dz, 0, 0, 0)), device_id_type=LOGICAL)
    with jax.named_scope("send_n2"):
        send_n_to(other)
        got_n[own, :] = send_n[own, :]
    with jax.named_scope("grad_z"):
        load_m.wait()
        deriv = (mats[0], mats[1])
        deriv_x = (mats[2], mats[3])
        for h in range(2):
            lay_out(send_g, h, matmul(deriv, split(turned[h])))
    with jax.named_scope("barrier_far"):
        pl.semaphore_wait(planes_sem, 3)
    with jax.named_scope("send_n_far"):
        send_n_to(far)
    with jax.named_scope("send_g"):
        send_all_chunks(send_g, got_g, 1, lambda i: chunk_sem.at[i], 1)

    moved = 8 * (ND - 1)
    with jax.named_scope("wait_n"):
        wait_all(got_n, recv_sem.at[0], moved)

    def turn_quad(block):
        return jnp.concatenate(block_turn([block[8 * b : 8 * b + 8] for b in range(4)]), axis=0)

    def lines_at(jk):
        return pl.ds(pl.multiple_of(jk * 32, 32), 32)

    def half_of(ref, kh):
        return jnp.concatenate([ref[kh, pl.ds(zz, N, stride=2), :] for zz in range(2)], axis=1)

    def rows_of(ref):
        return jnp.concatenate([ref[kh] for kh in range(2)], axis=1)

    with jax.named_scope("grad_xy"):
        for jk in range(2 * NJ):
            plane_n[jk % 2, 32 * (jk // 2) : 32 * (jk // 2) + 32, :] = turn_quad(got_n[32 * jk : 32 * jk + 32, :])
        along_y = matmul(split(rows_of(plane_n)), deriv)
        for kh in range(2):
            plane_y[kh] = -along_y[:, 128 * kh : 128 * kh + 128]
            along_x = matmul(deriv_x, split(half_of(plane_n, kh)))
            for zz in range(2):
                plane_x[kh, pl.ds(zz, N, stride=2), :] = along_x[:, 128 * zz : 128 * zz + 128]

    def cells(i, total, last):
        wait_all(got_g, chunk_sem.at[i], 120 if last else 128)
        quads = [base >> 2 for _, base in chunk_at(i, -1)]
        for group in GROUPS:
            group = [quads[q] for q in group]
            refs = [(jk & 1, lines_at(jk >> 1), slice(None)) for jk in group]
            n = jnp.concatenate([plane_n[r] for r in refs], axis=0)
            gx = jnp.concatenate([plane_x[r] for r in refs], axis=0)
            gy = jnp.concatenate([plane_y[r] for r in refs], axis=0)
            gz = jnp.concatenate([turn_quad(got_g[lines_at(jk), :]) for jk in group], axis=0)
            f, d_dens, slope = xc_parts(n, gx * gx + gy * gy + gz * gz)
            fx, fy, fz = slope * gx, slope * gy, slope * gz
            for g, jk in enumerate(group):
                send_f[lines_at(jk), :] = turn_quad(fz[32 * g : 32 * g + 32])
            for g, r in enumerate(refs):
                plane_d[r] = d_dens[32 * g : 32 * g + 32]
                plane_x[r] = fx[32 * g : 32 * g + 32]
                plane_y[r] = fy[32 * g : 32 * g + 32]
            for i8 in range(4 * len(group)):
                total = total + f[8 * i8 : 8 * i8 + 8]
        send_chunk(i, -1, last, lambda p: send_to(p, piece(send_f, p), got_f.at[own], 2, recv_sem.at[2]))
        return total

    with jax.named_scope("cells"):
        total = lax.fori_loop(0, CHUNKS - 1, functools.partial(cells, last=False), jnp.zeros((8, 128), F32))
        total = cells(CHUNKS - 1, total, last=True)
        mine = jnp.sum(total, axis=0, keepdims=True)
        e_own[0] = mine
        e_row[k] = mine
        got_f[own, :] = send_f[own, :]

    def send_row(i, carry):
        send_to(j * NK + ((k + i) & (NK - 1)), e_own.at[0], e_row.at[k], 4, recv_sem.at[4])
        return carry

    lax.fori_loop(1, NK, send_row, 0)

    def send_v_to(some):
        for step in some:
            p = at_step(step)
            send_to(p, piece(send_v, p), got_v.at[own], 3, recv_sem.at[3])

    flux_rows = split(rows_of(plane_y))
    v_sets = [[s for s in steps if s[1] % 2 == odd] for odd in range(2)]
    for odd in range(2):
        kh = (chip_y + odd) & 1
        with jax.named_scope("divergence"):
            half = pl.ds(pl.multiple_of(128 * kh, 128), 128)
            v_half = plane_d[kh] + matmul(flux_rows, (mats[0, :, half], mats[1, :, half]))
            along_x = matmul(deriv_x, split(half_of(plane_x, kh)))
            plane_d[kh] = v_half
            for zz in range(2):
                rows = (kh, pl.ds(zz, N, stride=2), slice(None))
                plane_d[rows] = plane_d[rows] - along_x[:, 128 * zz : 128 * zz + 128]
            for pj in range(NJ):
                send_v[lines_at(2 * pj + kh), :] = turn_quad(plane_d[kh, 32 * pj : 32 * pj + 32, :])
        with jax.named_scope("send_v"):
            send_v_to(v_sets[odd] if odd == 0 else v_sets[odd][:48])
    got_v[own, :] = send_v[own, :]

    with jax.named_scope("energy_row"):
        wait_all(e_row, recv_sem.at[4], NK - 1)
        row = jnp.sum(e_row[...], axis=0)
        e_mid[0] = row
        e_all[j] = row

        def send_col(i, carry):
            send_to(((j + i) & (NJ - 1)) * NK + k, e_mid.at[0], e_all.at[j], 5, recv_sem.at[5])
            return carry

        lax.fori_loop(1, NJ, send_col, 0)

    with jax.named_scope("send_v_end"):
        send_v_to(v_sets[1][48:])

    def gathered(ref, h):
        return jnp.concatenate(
            [
                jnp.concatenate([ref[pl.ds(2 * (2 * h + c) + zz, 128, stride=8), :] for c in range(2)], axis=1)
                for zz in range(2)
            ],
            axis=0,
        )

    with jax.named_scope("wait_f"):
        wait_all(got_f, recv_sem.at[2], moved)
    with jax.named_scope("div_z"):
        for h in range(2):
            div_z[h] = matmul(deriv, split(gathered(got_f, h)))
    with jax.named_scope("energy"):
        wait_all(e_all, recv_sem.at[5], NJ - 1)
        e_out[...] = jnp.full((8, 128), jnp.sum(jnp.sum(e_all[...], axis=0)) * (1.0 / N**3), F32)
        save_e = pltpu.make_async_copy(e_out, en_ref, load_sem.at[2])
        save_e.start()
    with jax.named_scope("sent"):
        for s, ref in enumerate((send_n, send_g, send_f)):
            wait_all(ref, send_sem.at[s], moved)
        wait_all(e_row, send_sem.at[4], NK - 1)
        wait_all(e_all, send_sem.at[5], NJ - 1)
    with jax.named_scope("wait_v"):
        wait_all(got_v, recv_sem.at[3], moved)
    with jax.named_scope("finish"):
        for h in range(2):
            out_ref[256 * h : 256 * h + 256, :] = (gathered(got_v, h) - div_z[h]).T

    wait_all(send_v, send_sem.at[3], moved)
    save_e.wait()


def store(p_ref, e_ref, p_hbm, e_hbm, scalar, sem):
    put_p = pltpu.make_async_copy(p_ref, p_hbm, sem.at[0])
    put_p.start()
    scalar[0, 0] = e_ref[0, 0]
    put_e = pltpu.make_async_copy(scalar, e_hbm, sem.at[1])
    put_e.start()
    put_p.wait()
    put_e.wait()


def body(density):
    flat = density.reshape(-1, density.shape[2])
    deriv = deriv_matrix()
    order = row_order()
    mats = np.stack(split_np(deriv) + split_np(deriv[order][:, order]))
    hbm = pl.BlockSpec(memory_space=pltpu.HBM)
    lines = pltpu.VMEM((ROWS, 128), F32)
    planes = pltpu.VMEM((2, 2 * N, 128), F32)
    potential, energy = pl.pallas_call(
        kernel,
        name="pbe",
        out_shape=(
            jax.ShapeDtypeStruct(flat.shape, F32),
            jax.ShapeDtypeStruct((8, 128), F32),
        ),
        in_specs=[hbm] * 2,
        out_specs=(pl.BlockSpec(memory_space=pltpu.VMEM), hbm),
        scratch_shapes=[pltpu.VMEM(flat.shape, F32), pltpu.VMEM((4, N, N), BF16)]
        + [lines] * 4
        + [planes] * 4
        + [lines] * 4
        + [
            pltpu.VMEM((2, N, N), F32),
            pltpu.VMEM((1, 1, 128), F32),
            pltpu.VMEM((NK, 1, 128), F32),
            pltpu.VMEM((1, 1, 128), F32),
            pltpu.VMEM((NJ, 1, 128), F32),
            pltpu.VMEM((8, 128), F32),
            pltpu.SemaphoreType.DMA((3,)),
            pltpu.SemaphoreType.DMA((6,)),
            pltpu.SemaphoreType.DMA((6,)),
            pltpu.SemaphoreType.DMA((NJ // 2,)),
            pltpu.SemaphoreType.REGULAR,
            pltpu.SemaphoreType.REGULAR,
        ],
        compiler_params=pltpu.CompilerParams(collective_id=0, has_side_effects=True, vmem_limit_bytes=40 * 2**20),
    )(*(pltpu.with_memory_space_constraint(a, pltpu.HBM) for a in (flat, jnp.asarray(mats))))
    potential, energy = pl.pallas_call(
        store,
        name="store",
        out_shape=(jax.ShapeDtypeStruct(flat.shape, F32), jax.ShapeDtypeStruct((1, 1), F32)),
        in_specs=[pl.BlockSpec(memory_space=pltpu.VMEM)] * 2,
        out_specs=(pl.BlockSpec(memory_space=pl.ANY), pl.BlockSpec(memory_space=pl.ANY)),
        scratch_shapes=[pltpu.SMEM((1, 1), F32), pltpu.SemaphoreType.DMA((2,))],
        compiler_params=pltpu.CompilerParams(vmem_limit_bytes=4 * 2**20),
    )(potential, energy)
    return potential.reshape(density.shape), energy[0, 0]


def solution(mesh):
    return jax.shard_map(
        body,
        mesh=mesh,
        in_specs=(P("gx", "gy", None),),
        out_specs=(P("gx", "gy", None), P()),
        check_vma=False,
    )
```

```python
import functools
import math

import jax
import jax.numpy as jnp
import numpy as np
from jax import lax
from jax.experimental import pallas as pl
from jax.experimental.pallas import tpu as pltpu
from jax.sharding import PartitionSpec as P

LOGICAL = pl.DeviceIdType.LOGICAL
F32 = jnp.float32
BF16 = jnp.bfloat16

N = 256
NJ = 16
NK = 8
ND = NJ * NK
ROWS = N * N * N // ND // 128

pbe_kappa = 0.804
pbe_mu = 0.2195149727645171
pbe_beta = 0.06672455060314922
pbe_gamma = 0.031090690869654894
pw_coef = 0.0310907
pw_alpha = 0.2137
pw_first = 7.5957
pw_second = 3.5876
pw_third = 1.6382
pw_fourth = 0.49294

kf_coef = (3.0 * math.pi**2) ** (1.0 / 3.0)
rs_coef = (3.0 / (4.0 * math.pi)) ** (1.0 / 3.0)


def deriv_matrix():
    m = np.arange(N)
    signed = np.where(m < N // 2, m, m - N)
    signed = np.where(m == N // 2, 0, signed) * (2.0 * math.pi / N)
    shift = (m[:, None] - m[None, :]) % N
    line = -(signed[None, :] * np.sin(2.0 * math.pi * (m[:, None] * m[None, :] % N) / N)).sum(1) / N
    return line[shift]


def row_order():
    r = np.arange(N)
    return 16 * (r // 16) + 4 * (r % 4) + (r // 4) % 4


def split_np(a):
    hi = a.astype(jnp.bfloat16)
    lo = (a - hi.astype(np.float64)).astype(jnp.bfloat16)
    return hi, lo


def split(a):
    hi = a.astype(BF16)
    lo = (a - hi.astype(F32)).astype(BF16)
    return hi, lo


def dot(a, b):
    return jnp.dot(a, b, preferred_element_type=F32)


def matmul(a, b):
    (ah, al), (bh, bl) = a, b
    return dot(ah, bh) + (dot(ah, bl) + dot(al, bh))


def xc_parts(n, g):
    w = jnp.exp(jnp.log(n) * (-1.0 / 6.0))
    w2 = w * w
    w4 = w2 * w2
    w6 = w4 * w2
    w14 = (w4 * w4) * w6
    cube = n * w4
    g14 = g * w14
    both_t = g14 * (pbe_beta / pbe_gamma * math.pi / (16.0 * kf_coef))
    s_scaled = (g14 * w2) * (pbe_mu / pbe_kappa / (4.0 * kf_coef**2))
    quot = 1.0 / (1.0 + s_scaled)
    c_x = -0.75 * kf_coef / math.pi
    cube_quot = cube * quot
    exch = cube * (c_x * (1.0 + pbe_kappa)) - cube_quot * (c_x * pbe_kappa)
    cube_quot2 = cube_quot * quot

    c2 = 2.0 * pw_coef
    r1 = math.sqrt(rs_coef)
    a1, a2, a3, a4 = c2 * pw_first * r1, c2 * pw_second * r1**2, c2 * pw_third * r1**3, c2 * pw_fourth * r1**4
    series = w * (a1 + w * (a2 + w * (a3 + w * a4)))
    series_rs = w * (0.5 * a1 + w * (a2 + w * (1.5 * a3 + w * (2.0 * a4))))
    series1 = series + 1.0
    inv_both = 1.0 / (series * series1)
    logarithm = jnp.log(1.0 + series1 * inv_both)
    alpha = w2 * (c2 * pw_alpha * rs_coef)
    lead = c2 + alpha
    minus_corr = lead * logarithm
    corr_rs = lead * (series_rs * inv_both) - alpha * logarithm

    grown = jnp.exp(minus_corr * (1.0 / pbe_gamma))
    inv_e = 1.0 / (grown - 1.0)
    y = inv_e * both_t
    y1 = 1.0 + y
    yy = y * y
    den = y1 + yy
    both = den + both_t * y1
    inv = 1.0 / (den * both)
    term = pbe_gamma * jnp.log(both * both * inv)
    slope_t = (y1 + y) * inv
    term_t = (both_t * slope_t) * (-7.0 / 3.0 * pbe_gamma)
    term_c = ((yy * both_t) * (1.0 + y1)) * ((inv * inv_e) * grown)

    per_cell = (exch - minus_corr) + term
    exch_s = (cube_quot2 * s_scaled) * (-8.0 / 3.0 * c_x * pbe_kappa)
    d_dens = per_cell + (exch - corr_rs * (1.0 - term_c)) * (1.0 / 3.0) + (exch_s + term_t)
    twice_d_grad = (n * w14) * (
        (cube_quot2 * w2) * (2.0 * c_x * pbe_mu / (4.0 * kf_coef**2))
        + slope_t * (2.0 * pbe_beta * math.pi / (16.0 * kf_coef))
    )
    return n * per_cell, d_dens, twice_d_grad


def block_turn(parts):
    group = lax.broadcasted_iota(jnp.int32, parts[0].shape, 1) // 32
    turned = [parts[0]] + [pltpu.roll(parts[b], 32 * b, 1) for b in range(1, 4)]
    out = []
    for a in range(4):
        mixed = jnp.where(
            group < 2,
            jnp.where(group == 0, turned[-a % 4], turned[(1 - a) % 4]),
            jnp.where(group == 2, turned[(2 - a) % 4], turned[(3 - a) % 4]),
        )
        out.append(mixed if a == 0 else pltpu.roll(mixed, 128 - 32 * a, 1))
    return out


FAR_FIRST = (2, 1, 3, 0)
CHUNKS = 8
GROUPS = ((0, 1, 2, 3),)


def kernel(
    f_hbm, mats_hbm, out_ref, en_ref,
    f_ref, mats,
    send_n, send_g, got_n, got_g, plane_n, plane_x, plane_y, plane_d,
    send_f, send_v, got_f, got_v, div_z, e_own, e_row, e_mid, e_all, e_out,
    load_sem, send_sem, recv_sem, chunk_sem, planes_sem, half_sem,
):
    j = lax.axis_index("gx")
    k = lax.axis_index("gy")
    me = j * NK + k
    own = pl.ds(pl.multiple_of(me * 8, 8), 8)
    chip_z, core, chip_x = j >> 2, j & 1, k & 3
    chip_y = (j & 2) + (k >> 2)
    at_z = [((chip_z + d) & 3) << 5 for d in range(4)]
    at_x = [(chip_x + d) & 3 for d in range(4)]

    def at_y(d):
        y = (chip_y + d) & 3
        return ((y & 2) << 3) + ((y & 1) << 2)

    load_f = pltpu.make_async_copy(f_hbm, f_ref, load_sem.at[0])
    load_m = pltpu.make_async_copy(mats_hbm, mats, load_sem.at[1])
    all_y = [at_y(d) for d in range(4)]
    cores = [core << 3, (1 - core) << 3]
    steps = [(dz, dy, dx, dc) for dz in range(4) for dy in range(4) for dx in range(4) for dc in range(2)][1:]
    steps = sorted(steps, key=lambda s: (-sum(min(d, 4 - d) for d in s[:3]), s))
    near = [s for s in steps if 0 in s[:3]]
    far = [s for s in steps if 0 not in s[:3]]

    def at_step(s):
        return at_z[s[0]] + all_y[s[1]] + cores[s[3]] + at_x[s[2]]

    same = [s for s in near if s[3] == 0]
    other = [s for s in near if s[3] == 1]
    barrier = pltpu.get_barrier_semaphore()
    with jax.named_scope("greet"):
        for s in other[-1:] + same:
            pl.semaphore_signal(barrier, inc=1, device_id=at_step(s), device_id_type=LOGICAL)
        load_f.start()
        load_m.start()

    def chunk_at(i, sign):
        turn = i + 1
        side = (core ^ ((turn >> 2) & 1)) << 3
        return [(d, at_z[sign * d % 4] + at_y(sign * (d + turn)) + side) for d in FAR_FIRST]

    def send_chunk(i, sign, last, one):
        for d, base in chunk_at(i, sign):
            for dx in FAR_FIRST:
                if not (last and d == 0 and dx == 0):
                    one(base + at_x[dx])

    def send_to(p, src, dst, s, r):
        pltpu.make_async_remote_copy(
            src_ref=src, dst_ref=dst, send_sem=send_sem.at[s], recv_sem=r, device_id=p, device_id_type=LOGICAL
        ).start()

    def piece(ref, p):
        return ref.at[pl.ds(pl.multiple_of(p * 8, 8), 8)]

    def send_all_chunks(src, dst, s, sem_of, sign):
        def chunk(i, carry):
            send_chunk(i, sign, False, lambda p: send_to(p, piece(src, p), dst.at[own], s, sem_of(i)))
            return carry

        lax.fori_loop(0, CHUNKS - 1, chunk, 0)
        i = CHUNKS - 1
        send_chunk(i, sign, True, lambda p: send_to(p, piece(src, p), dst.at[own], s, sem_of(i)))
        dst[own, :] = src[own, :]

    def wait_all(ref, sem, rows):
        part = ref.at[pl.ds(0, rows)]
        pltpu.make_async_copy(part, part, sem).wait()

    def lay_out(ref, h, block):
        for c in range(2):
            for zz in range(2):
                ref[pl.ds(2 * (2 * h + c) + zz, 128, stride=8), :] = block[
                    128 * zz : 128 * zz + 128, 128 * c : 128 * c + 128
                ]

    with jax.named_scope("load"):
        load_f.wait()
        turned = [f_ref[256 * h : 256 * h + 256, :].T for h in range(2)]
        for h in range(2):
            lay_out(send_n, h, turned[h])
    def send_n_to(some):
        for s in some:
            p = at_step(s)
            send_to(p, piece(send_n, p), got_n.at[own], 0, recv_sem.at[0])

    with jax.named_scope("barrier"):
        pl.semaphore_wait(barrier, len(same) + 1)
        pl.semaphore_signal(half_sem, inc=1, device_id=at_step((0, 0, 0, 1)), device_id_type=LOGICAL)
    with jax.named_scope("send_n"):
        send_n_to(same)
    with jax.named_scope("barrier_half"):
        pl.semaphore_wait(half_sem, 1)
        for dz in (2, 1, 3):
            pl.semaphore_signal(planes_sem, inc=1, device_id=at_step((dz, 0, 0, 0)), device_id_type=LOGICAL)
    with jax.named_scope("send_n2"):
        send_n_to(other)
        got_n[own, :] = send_n[own, :]
    with jax.named_scope("grad_z"):
        load_m.wait()
        deriv = (mats[0], mats[1])
        deriv_x = (mats[2], mats[3])
        for h in range(2):
            lay_out(send_g, h, matmul(deriv, split(turned[h])))
    with jax.named_scope("barrier_far"):
        pl.semaphore_wait(planes_sem, 3)
    with jax.named_scope("send_n_far"):
        send_n_to(far)
    with jax.named_scope("send_g"):
        send_all_chunks(send_g, got_g, 1, lambda i: chunk_sem.at[i], 1)

    moved = 8 * (ND - 1)
    with jax.named_scope("wait_n"):
        wait_all(got_n, recv_sem.at[0], moved)

    def turn_quad(block):
        return jnp.concatenate(block_turn([block[8 * b : 8 * b + 8] for b in range(4)]), axis=0)

    def lines_at(jk):
        return pl.ds(pl.multiple_of(jk * 32, 32), 32)

    def half_of(ref, kh):
        return jnp.concatenate([ref[kh, pl.ds(zz, N, stride=2), :] for zz in range(2)], axis=1)

    def rows_of(ref):
        return jnp.concatenate([ref[kh] for kh in range(2)], axis=1)

    with jax.named_scope("grad_xy"):
        for jk in range(2 * NJ):
            plane_n[jk % 2, 32 * (jk // 2) : 32 * (jk // 2) + 32, :] = turn_quad(got_n[32 * jk : 32 * jk + 32, :])
        along_y = matmul(split(rows_of(plane_n)), deriv)
        for kh in range(2):
            plane_y[kh] = -along_y[:, 128 * kh : 128 * kh + 128]
            along_x = matmul(deriv_x, split(half_of(plane_n, kh)))
            for zz in range(2):
                plane_x[kh, pl.ds(zz, N, stride=2), :] = along_x[:, 128 * zz : 128 * zz + 128]

    def cells(i, total, last):
        wait_all(got_g, chunk_sem.at[i], 120 if last else 128)
        quads = [base >> 2 for _, base in chunk_at(i, -1)]
        for group in GROUPS:
            group = [quads[q] for q in group]
            refs = [(jk & 1, lines_at(jk >> 1), slice(None)) for jk in group]
            n = jnp.concatenate([plane_n[r] for r in refs], axis=0)
            gx = jnp.concatenate([plane_x[r] for r in refs], axis=0)
            gy = jnp.concatenate([plane_y[r] for r in refs], axis=0)
            gz = jnp.concatenate([turn_quad(got_g[lines_at(jk), :]) for jk in group], axis=0)
            f, d_dens, slope = xc_parts(n, gx * gx + gy * gy + gz * gz)
            fx, fy, fz = slope * gx, slope * gy, slope * gz
            for g, jk in enumerate(group):
                send_f[lines_at(jk), :] = turn_quad(fz[32 * g : 32 * g + 32])
            for g, r in enumerate(refs):
                plane_d[r] = d_dens[32 * g : 32 * g + 32]
                plane_x[r] = fx[32 * g : 32 * g + 32]
                plane_y[r] = fy[32 * g : 32 * g + 32]
            for i8 in range(4 * len(group)):
                total = total + f[8 * i8 : 8 * i8 + 8]
        send_chunk(i, -1, last, lambda p: send_to(p, piece(send_f, p), got_f.at[own], 2, recv_sem.at[2]))
        return total

    with jax.named_scope("cells"):
        total = lax.fori_loop(0, CHUNKS - 1, functools.partial(cells, last=False), jnp.zeros((8, 128), F32))
        total = cells(CHUNKS - 1, total, last=True)
        mine = jnp.sum(total, axis=0, keepdims=True)
        e_own[0] = mine
        e_row[k] = mine
        got_f[own, :] = send_f[own, :]

    def send_row(i, carry):
        send_to(j * NK + ((k + i) & (NK - 1)), e_own.at[0], e_row.at[k], 4, recv_sem.at[4])
        return carry

    lax.fori_loop(1, NK, send_row, 0)

    def send_v_to(some):
        for step in some:
            p = at_step(step)
            send_to(p, piece(send_v, p), got_v.at[own], 3, recv_sem.at[3])

    flux_rows = split(rows_of(plane_y))
    v_sets = [[s for s in steps if s[1] % 2 == odd] for odd in range(2)]
    for odd in range(2):
        kh = (chip_y + odd) & 1
        with jax.named_scope("divergence"):
            half = pl.ds(pl.multiple_of(128 * kh, 128), 128)
            v_half = plane_d[kh] + matmul(flux_rows, (mats[0, :, half], mats[1, :, half]))
            along_x = matmul(deriv_x, split(half_of(plane_x, kh)))
            plane_d[kh] = v_half
            for zz in range(2):
                rows = (kh, pl.ds(zz, N, stride=2), slice(None))
                plane_d[rows] = plane_d[rows] - along_x[:, 128 * zz : 128 * zz + 128]
            for pj in range(NJ):
                send_v[lines_at(2 * pj + kh), :] = turn_quad(plane_d[kh, 32 * pj : 32 * pj + 32, :])
        with jax.named_scope("send_v"):
            send_v_to(v_sets[odd] if odd == 0 else v_sets[odd][:48])
    got_v[own, :] = send_v[own, :]

    with jax.named_scope("energy_row"):
        wait_all(e_row, recv_sem.at[4], NK - 1)
        row = jnp.sum(e_row[...], axis=0)
        e_mid[0] = row
        e_all[j] = row

        def send_col(i, carry):
            send_to(((j + i) & (NJ - 1)) * NK + k, e_mid.at[0], e_all.at[j], 5, recv_sem.at[5])
            return carry

        lax.fori_loop(1, NJ, send_col, 0)

    with jax.named_scope("send_v_end"):
        send_v_to(v_sets[1][48:])

    def gathered(ref, h):
        return jnp.concatenate(
            [
                jnp.concatenate([ref[pl.ds(2 * (2 * h + c) + zz, 128, stride=8), :] for c in range(2)], axis=1)
                for zz in range(2)
            ],
            axis=0,
        )

    with jax.named_scope("wait_f"):
        wait_all(got_f, recv_sem.at[2], moved)
    with jax.named_scope("div_z"):
        for h in range(2):
            div_z[h] = matmul(deriv, split(gathered(got_f, h)))
    with jax.named_scope("energy"):
        wait_all(e_all, recv_sem.at[5], NJ - 1)
        e_out[...] = jnp.full((8, 128), jnp.sum(jnp.sum(e_all[...], axis=0)) * (1.0 / N**3), F32)
        save_e = pltpu.make_async_copy(e_out, en_ref, load_sem.at[2])
        save_e.start()
    with jax.named_scope("sent"):
        for s, ref in enumerate((send_n, send_g, send_f)):
            wait_all(ref, send_sem.at[s], moved)
        wait_all(e_row, send_sem.at[4], NK - 1)
        wait_all(e_all, send_sem.at[5], NJ - 1)
    with jax.named_scope("wait_v"):
        wait_all(got_v, recv_sem.at[3], moved)
    with jax.named_scope("finish"):
        for h in range(2):
            out_ref[256 * h : 256 * h + 256, :] = (gathered(got_v, h) - div_z[h]).T

    wait_all(send_v, send_sem.at[3], moved)
    save_e.wait()


def store(p_ref, e_ref, p_hbm, e_hbm, scalar, sem):
    put_p = pltpu.make_async_copy(p_ref, p_hbm, sem.at[0])
    put_p.start()
    scalar[0, 0] = e_ref[0, 0]
    put_e = pltpu.make_async_copy(scalar, e_hbm, sem.at[1])
    put_e.start()
    put_p.wait()
    put_e.wait()


def body(density):
    flat = density.reshape(-1, density.shape[2])
    deriv = deriv_matrix()
    order = row_order()
    mats = np.stack(split_np(deriv) + split_np(deriv[order][:, order]))
    hbm = pl.BlockSpec(memory_space=pltpu.HBM)
    lines = pltpu.VMEM((ROWS, 128), F32)
    planes = pltpu.VMEM((2, 2 * N, 128), F32)
    potential, energy = pl.pallas_call(
        kernel,
        name="pbe",
        out_shape=(
            jax.ShapeDtypeStruct(flat.shape, F32),
            jax.ShapeDtypeStruct((8, 128), F32),
        ),
        in_specs=[hbm] * 2,
        out_specs=(pl.BlockSpec(memory_space=pltpu.VMEM), hbm),
        scratch_shapes=[pltpu.VMEM(flat.shape, F32), pltpu.VMEM((4, N, N), BF16)]
        + [lines] * 4
        + [planes] * 4
        + [lines] * 4
        + [
            pltpu.VMEM((2, N, N), F32),
            pltpu.VMEM((1, 1, 128), F32),
            pltpu.VMEM((NK, 1, 128), F32),
            pltpu.VMEM((1, 1, 128), F32),
            pltpu.VMEM((NJ, 1, 128), F32),
            pltpu.VMEM((8, 128), F32),
            pltpu.SemaphoreType.DMA((3,)),
            pltpu.SemaphoreType.DMA((6,)),
            pltpu.SemaphoreType.DMA((6,)),
            pltpu.SemaphoreType.DMA((NJ // 2,)),
            pltpu.SemaphoreType.REGULAR,
            pltpu.SemaphoreType.REGULAR,
        ],
        compiler_params=pltpu.CompilerParams(collective_id=0, has_side_effects=True, vmem_limit_bytes=40 * 2**20),
    )(*(pltpu.with_memory_space_constraint(a, pltpu.HBM) for a in (flat, jnp.asarray(mats))))
    potential, energy = pl.pallas_call(
        store,
        name="store",
        out_shape=(jax.ShapeDtypeStruct(flat.shape, F32), jax.ShapeDtypeStruct((1, 1), F32)),
        in_specs=[pl.BlockSpec(memory_space=pltpu.VMEM)] * 2,
        out_specs=(pl.BlockSpec(memory_space=pl.ANY), pl.BlockSpec(memory_space=pl.ANY)),
        scratch_shapes=[pltpu.SMEM((1, 1), F32), pltpu.SemaphoreType.DMA((2,))],
        compiler_params=pltpu.CompilerParams(vmem_limit_bytes=4 * 2**20),
    )(potential, energy)
    return potential.reshape(density.shape), energy[0, 0]


def solution(mesh):
    return jax.shard_map(
        body,
        mesh=mesh,
        in_specs=(P("gx", "gy", None),),
        out_specs=(P("gx", "gy", None), P()),
        check_vma=False,
    )
```
